128 devices in a mesh: data: 1, col: 64 (over z, y, x), dap: 2 (over core).
Axes of the slice: x: 4, y: 4, z: 4, core: 2. Of those that a mesh axis runs over, the one named last changes fastest.
Arguments:
- msa_act: bfloat16 [1024, 768, 256], P(('data', 'dap'), 'col')
- msa_mask: int32 [1024, 768], P(('data', 'dap'), 'col')
- pair_act: float32 [768, 768, 128], P(('data', 'dap'), 'col')
- ln_gamma: bfloat16 [256], replicated
- ln_beta: bfloat16 [256], replicated
- w_a: bfloat16 [256, 32], replicated
- b_a: bfloat16 [32], replicated
- w_b: bfloat16 [256, 32], replicated
- b_b: bfloat16 [32], replicated
- w_out: bfloat16 [1024, 128], replicated
- b_out: bfloat16 [128], replicated
Outputs:
- output: float32 [768, 768, 128], P(('data', 'dap'), 'col')
All inputs are finite; a program needn't handle non-finite values.
Results may differ from the reference program's by a relative error of at most 0.00129929.
Values are sent between devices in bfloat16 or wider.
A program may use at most 1 GiB of HBM per device.

```python
import jax
import jax.numpy as jnp
from jax import lax

NUM_SEQS = 1024
SHARD_SEQS = 512
NUM_RES = 768
MSA_DIM = 256
PAIR_DIM = 128
OPM_DIM = 32
ROW_BLOCK = 8


def draw_mask(mask_key):
    mask_keys = jax.random.split(mask_key, 5)
    starts = jax.random.randint(mask_keys[0], (NUM_SEQS, 1), 0, NUM_RES // 2)
    span_len = jax.random.randint(mask_keys[1], (NUM_SEQS, 1), NUM_RES // 4, NUM_RES + 1)
    res_idx = jnp.arange(NUM_RES)[None, :]
    in_window = (res_idx >= starts) & (res_idx < starts + span_len)
    levels = jax.random.randint(mask_keys[2], (NUM_SEQS // SHARD_SEQS, 1), 2, 9)
    keep_draw = jax.random.randint(mask_keys[3], (NUM_SEQS // SHARD_SEQS, SHARD_SEQS), 0, 8)
    seq_kept = (keep_draw < levels).reshape(NUM_SEQS, 1)
    res_kept = jax.random.randint(mask_keys[4], (NUM_SEQS, NUM_RES), 0, 8) > 0
    seq_idx = jnp.arange(NUM_SEQS)[:, None]
    return jnp.where(seq_idx == 0, 1, (in_window & seq_kept & res_kept).astype(jnp.int32)).astype(jnp.int32)


def setup_inputs(seed: int = 0, part: int = 0) -> dict:
    base_key = jax.random.key(seed)
    part_key = jax.random.fold_in(base_key, part)
    act_keys = jax.random.split(part_key, 3)
    weight_keys = jax.random.split(base_key, 8)
    coh_scale = 0.8 * NUM_SEQS ** -0.25
    msa_act = jax.random.normal(act_keys[0], (NUM_SEQS, NUM_RES, MSA_DIM), jnp.float32).astype(jnp.bfloat16)
    msa_mask = draw_mask(act_keys[1])
    pair_act = jax.random.normal(act_keys[2], (NUM_RES, NUM_RES, PAIR_DIM), jnp.float32)
    ln_gamma = (1.0 + 0.5 * jax.random.normal(weight_keys[0], (MSA_DIM,), jnp.float32)).astype(jnp.bfloat16)
    ln_beta = (coh_scale * jax.random.normal(weight_keys[1], (MSA_DIM,), jnp.float32)).astype(jnp.bfloat16)
    w_a = (jax.random.normal(weight_keys[2], (MSA_DIM, OPM_DIM), jnp.float32) * MSA_DIM ** -0.5).astype(jnp.bfloat16)
    b_a = (coh_scale * jax.random.normal(weight_keys[3], (OPM_DIM,), jnp.float32)).astype(jnp.bfloat16)
    w_b = (jax.random.normal(weight_keys[4], (MSA_DIM, OPM_DIM), jnp.float32) * MSA_DIM ** -0.5).astype(jnp.bfloat16)
    b_b = (coh_scale * jax.random.normal(weight_keys[5], (OPM_DIM,), jnp.float32)).astype(jnp.bfloat16)
    w_out = (jax.random.normal(weight_keys[6], (OPM_DIM * OPM_DIM, PAIR_DIM), jnp.float32) * (NUM_SEQS ** 0.5 / OPM_DIM)).astype(jnp.bfloat16)
    b_out = (jax.random.normal(weight_keys[7], (PAIR_DIM,), jnp.float32) * (0.3 * NUM_SEQS)).astype(jnp.bfloat16)
    return {'msa_act': msa_act, 'msa_mask': msa_mask, 'pair_act': pair_act, 'ln_gamma': ln_gamma, 'ln_beta': ln_beta, 'w_a': w_a, 'b_a': b_a, 'w_b': w_b, 'b_b': b_b, 'w_out': w_out, 'b_out': b_out}


def layer_norm(msa_act, ln_gamma, ln_beta):
    values_f = msa_act.astype(jnp.float32)
    mean_val = jnp.mean(values_f, axis=-1, keepdims=True)
    centred = values_f - mean_val
    variance = jnp.mean(centred * centred, axis=-1, keepdims=True)
    normed = centred * lax.rsqrt(variance + 1e-5)
    return (normed * ln_gamma.astype(jnp.float32) + ln_beta.astype(jnp.float32)).astype(jnp.bfloat16)


def reference(msa_act, msa_mask, pair_act, ln_gamma, ln_beta, w_a, b_a, w_b, b_b, w_out, b_out):
    normed = layer_norm(msa_act, ln_gamma, ln_beta)
    mask_f = msa_mask.astype(jnp.float32)
    flat_x = normed.reshape(NUM_SEQS * NUM_RES, MSA_DIM)
    lin_a = jnp.dot(flat_x, w_a, preferred_element_type=jnp.float32).reshape(NUM_SEQS, NUM_RES, OPM_DIM)
    lin_b = jnp.dot(flat_x, w_b, preferred_element_type=jnp.float32).reshape(NUM_SEQS, NUM_RES, OPM_DIM)
    proj_a = ((lin_a + b_a.astype(jnp.float32)) * mask_f[:, :, None]).astype(jnp.bfloat16).astype(jnp.float32)
    proj_b = ((lin_b + b_b.astype(jnp.float32)) * mask_f[:, :, None]).astype(jnp.bfloat16).astype(jnp.float32)
    w_flat = w_out.astype(jnp.float32)
    row_blocks = proj_a.reshape(NUM_SEQS, NUM_RES // ROW_BLOCK, ROW_BLOCK, OPM_DIM).transpose(1, 0, 2, 3)

    def block_fn(row_a):
        outer = jnp.einsum('sic,sjd->ijcd', row_a, proj_b)
        flat_outer = outer.reshape(ROW_BLOCK * NUM_RES, OPM_DIM * OPM_DIM)
        return jnp.dot(flat_outer, w_flat, preferred_element_type=jnp.float32).reshape(ROW_BLOCK, NUM_RES, PAIR_DIM)

    proj_sum = lax.map(block_fn, row_blocks).reshape(NUM_RES, NUM_RES, PAIR_DIM)
    pair_norm = jnp.dot(mask_f.T, mask_f, preferred_element_type=jnp.float32)
    return pair_act + (proj_sum + b_out.astype(jnp.float32)) / (1e-3 + pair_norm)[:, :, None]
```

```python
import jax
import jax.numpy as jnp
from jax import lax
from jax.experimental import pallas as pl
from jax.experimental.pallas import tpu as pltpu
from jax.sharding import PartitionSpec as P

F32 = jnp.float32
BF16 = jnp.bfloat16
MESH = pl.DeviceIdType.MESH
NT = (((1,), (1,)), ((), ()))

SEQ, RES, CH, HID, PAIR = 512, 12, 256, 32, 128
PIECE = 128
NP = SEQ // PIECE
AROWS = RES * HID
PROWS = AROWS + 16
UNIT = 2 * RES


def iota(shape, axis):
    return lax.broadcasted_iota(jnp.int32, shape, axis)


def dot(a, b, dims=None):
    if dims is None:
        return jnp.dot(a, b, preferred_element_type=F32)
    return lax.dot_general(a, b, dims, preferred_element_type=F32)


def kernel(m_hbm, mask_ref, z_hbm, gamma_ref, beta_ref, wa_ref, ba_ref, wb_ref, bb_ref, wo_ref, bo_ref,
           out_hbm,
           m_v, mask_v, wabig, b32, a_buf, b_buf, bt, lhs2, rt, w32, wo_p, r_send, r_recv, n_send, n_recv,
           mask_all, inv_v, z_v, out_v,
           m_sem, z_sem, o_sem, a_ss, a_rs, b_ss, b_rs, r_ss, r_rs, n_ss, n_rs):
    col = lax.axis_index("col")
    dap = lax.axis_index("dap")
    zz, yy, xx = col // 16, (col // 4) % 4, col % 4
    home = zz // 2
    other = 1 - dap

    def at(dz=0, dy=0, dx=0):
        return ((zz + dz) % 4) * 16 + ((yy + dy) % 4) * 4 + (xx + dx) % 4

    def dev(c, d):
        return {"col": c, "dap": d}

    for p in range(NP):
        pltpu.make_async_copy(m_hbm.at[:, pl.ds(PIECE * p, PIECE), :], m_v.at[p], m_sem.at[p]).start()
    barrier = pltpu.get_barrier_semaphore()
    greet = [dev(at(dy=1), dap), dev(at(dy=3), dap), dev(at(dx=1), dap), dev(at(dx=3), dap), dev(col, other)]
    for r in (1, 2, 3):
        for d in (0, 1):
            greet.append(dev(at(dz=r), d))
    for who in greet:
        pl.semaphore_signal(barrier, inc=1, device_id=who, device_id_type=MESH)

    mask_v[...] = jnp.zeros_like(mask_v)
    mask_v[0:RES, :] = mask_ref[...].astype(F32)
    wa = wa_ref[...]
    for k in range(4):
        rows = [wa if kk == k else jnp.zeros_like(wa) for kk in range(4)]
        wabig[:, CH * k:CH * (k + 1)] = jnp.concatenate(rows, axis=0)
    gamma = gamma_ref[...].astype(F32)
    beta = beta_ref[...].astype(F32)
    tile4 = jnp.where(iota((HID, 128), 1) % HID == iota((HID, 128), 0), 1.0, 0.0).astype(BF16)
    ba_row = dot(jnp.broadcast_to(ba_ref[...], (16, HID)), tile4)[0:1, :]
    eye = iota((HID, HID), 0) == iota((HID, HID), 1)
    bb_diag = jnp.where(eye, jnp.broadcast_to(bb_ref[...], (HID, HID)).astype(F32), 0.0).astype(BF16)
    bb_col = dot(bb_diag, jnp.ones((HID, 128), BF16))

    def a_copy(slot, p, way):
        dy, dx = slot
        sy, sx = {"x+": (0, 1), "x-": (0, -1), "y+": (1, 0), "y-": (-1, 0)}[way]
        to = ((dy + sy) % 4) * 4 + (dx + sx) % 4
        w = {"x+": 0, "x-": 1, "y+": 2, "y-": 3}[way]
        here = dy * 4 + dx
        return pltpu.make_async_remote_copy(
            src_ref=a_buf.at[here, p], dst_ref=a_buf.at[to, p], send_sem=a_ss.at[here, p, w],
            recv_sem=a_rs.at[to, p], device_id=dev(at(dy=sy, dx=sx), dap), device_id_type=MESH)

    def b_copy(r, p, way):
        s = 1 if way == "z+" else -1
        to = (r + s) % 4
        return pltpu.make_async_remote_copy(
            src_ref=b_buf.at[r, p], dst_ref=b_buf.at[to, p], send_sem=b_ss.at[r, p, 0 if s == 1 else 1],
            recv_sem=b_rs.at[to, p], device_id=dev(at(dz=s), dap), device_id_type=MESH)

    a_sent, b_sent = [], []

    def send_a(slot, p, way):
        a_copy(slot, p, way).start()
        a_sent.append((slot, p, way))

    def send_b(r, p, way):
        b_copy(r, p, way).start()
        b_sent.append((r, p, way))

    def wait_a(slot, p):
        i = slot[0] * 4 + slot[1]
        pltpu.make_async_remote_copy(
            src_ref=a_buf.at[i, p], dst_ref=a_buf.at[i, p], send_sem=a_ss.at[i, p, 0], recv_sem=a_rs.at[i, p],
            device_id=dev(at(dx=1), dap), device_id_type=MESH).wait_recv()

    def wait_b(r, p):
        pltpu.make_async_remote_copy(
            src_ref=b_buf.at[r, p], dst_ref=b_buf.at[r, p], send_sem=b_ss.at[r, p, 0], recv_sem=b_rs.at[r, p],
            device_id=dev(at(dz=1), dap), device_id_type=MESH).wait_recv()

    def project(p, carry):
        pltpu.make_async_copy(m_hbm.at[:, pl.ds(0, PIECE), :], m_v.at[p], m_sem.at[p]).wait()
        lanes = pl.ds(pl.multiple_of(PIECE * p, PIECE), PIECE)
        mask_p = mask_v[:, lanes]
        mask_b = mask_p.astype(BF16)
        mask_t = mask_p.T.astype(BF16)
        for q in range(3):
            xs = []
            for k in range(4):
                n = 4 * q + k
                v = m_v[p, n].astype(F32)
                mean = jnp.sum(v, axis=1, keepdims=True) * (1.0 / CH)
                cen = v - mean
                var = jnp.sum(cen * cen, axis=1, keepdims=True) * (1.0 / CH)
                x = (cen * lax.rsqrt(var + 1e-5) * gamma + beta).astype(BF16)
                xs.append(x)
                lin_b = dot(wb_ref[...], x, NT)
                b32[pl.ds(n, HID, stride=RES), :] = (lin_b + bb_col) * mask_p[n:n + 1, :]
            lin_a = dot(jnp.concatenate(xs, axis=1), wabig[...], NT)
            spread = jnp.where(iota((16, 128), 1) // HID + 4 * q == iota((16, 128), 0), 1.0, 0.0).astype(BF16)
            a_buf[0, p, 128 * q:128 * (q + 1), :] = ((lin_a + ba_row) * dot(mask_t, spread)).astype(BF16)
        a_buf[0, p, AROWS:PROWS, :] = mask_b
        b_buf[0, p, 0:AROWS, :] = b32[...].astype(BF16)
        b_buf[0, p, AROWS:PROWS, :] = mask_b

        @pl.when(p == 0)
        def _():
            pl.semaphore_wait(barrier, len(greet))

        for way in ("z+", "z-"):
            b_copy(0, p, way).start()
        for way in ("x+", "x-", "y+", "y-"):
            a_copy((0, 0), p, way).start()
        return carry

    lax.fori_loop(0, NP, project, 0)
    for p in range(NP):
        b_sent += [(0, p, w) for w in ("z+", "z-")]
        a_sent += [((0, 0), p, w) for w in ("x+", "x-", "y+", "y-")]
    pltpu.make_async_copy(z_hbm, z_v, z_sem).start()

    early = []
    for p in (0, 1):
        wait_b(1, p)
        send_b(1, p, "z+")
        wait_b(3, p)
    for p in range(NP):
        fwd = p // 2 == 0
        if p >= 2:
            wait_b(3, p)
            send_b(3, p, "z-")
            wait_b(1, p)
        for d, on in ((1, "+"), (3, "-")):
            slot = (0, d) if p % 2 == 0 else (d, 0)
            wait_a(slot, p)
            early.append((slot, p))
            first, second = ("x", "y") if p % 2 == 0 else ("y", "x")
            if fwd == (d == 1):
                send_a(slot, p, first + on)
            send_a(slot, p, second + "+")
            send_a(slot, p, second + "-")

    w32[...] = wo_ref[...].astype(F32)

    def order(d, carry):
        wo_p[pl.ds(pl.multiple_of(HID * d, HID), HID), :] = w32[pl.ds(d, HID, stride=HID), :].astype(BF16)
        return carry

    lax.fori_loop(0, HID, order, 0)

    for p in range(NP):
        slot = (0, 2) if p % 2 == 0 else (2, 0)
        second = "y" if p % 2 == 0 else "x"
        wait_a(slot, p)
        early.append((slot, p))
        send_a(slot, p, second + "+")
        send_a(slot, p, second + "-")

    for p in range(NP):
        wait_b(2, p)
    n192 = 4 * 4 * RES
    ro, co = iota((n192, n192), 0), iota((n192, n192), 1)
    want = ((ro // RES) % 4) * 48 + (ro // 48) * RES + ro % RES
    perm = jnp.where(want == co, 1.0, 0.0).astype(BF16)

    def regroup(g, carry):
        rows = pl.ds(pl.multiple_of(48 * g, 16), 48)
        cat = jnp.concatenate(
            [jnp.concatenate([b_buf[r, p, rows, :] for p in range(NP)], axis=1) for r in range(4)], axis=0)
        bt[pl.ds(pl.multiple_of(n192 * g, 64), n192), :] = dot(perm, cat).astype(BF16)
        return carry

    lax.fori_loop(0, 8, regroup, 0)

    lane = iota((1, 128), 1)
    low = lane < 64
    odd = (lane // HID) % 2 == 1

    def transpose4(v):
        def swap(u, w):
            t = pltpu.roll(jnp.where(low, w, u), 64, 1)
            return jnp.where(low, u, t), jnp.where(low, t, w)

        def swap2(u, w):
            return (jnp.where(odd, pltpu.roll(w, 32, 1), u), jnp.where(odd, w, pltpu.roll(u, 96, 1)))

        e0, e2 = swap(v[0], v[2])
        e1, e3 = swap(v[1], v[3])
        w0, w1 = swap2(e0, e1)
        w2, w3 = swap2(e2, e3)
        return w0, w1, w2, w3

    def r_copy(t, r, unit):
        return pltpu.make_async_remote_copy(
            src_ref=r_send.at[t, r], dst_ref=r_recv.at[zz % 2, dap, unit], send_sem=r_ss.at[t, r],
            recv_sem=r_rs.at[zz % 2, dap, unit], device_id=dev(at(dz=-r), home), device_id_type=MESH)

    def n_copy(r):
        return pltpu.make_async_remote_copy(
            src_ref=n_send.at[r], dst_ref=n_recv.at[zz % 2, dap], send_sem=n_ss.at[r],
            recv_sem=n_rs.at[zz % 2, dap], device_id=dev(at(dz=-r), home), device_id_type=MESH)

    line = (0, 1, 3, 2)
    done = set(early)
    plan = {0: [], 2: [], 4: [], 6: []}
    for i, dy in enumerate(line):
        for dx in (0, 1, 3, 2):
            for p in range(NP):
                if (dy, dx) == (0, 0) or ((dy, dx), p) in done:
                    continue
                h, e = p % 2, p // 2
                on = None
                if h == 0 and dy == 1 and e == 0:
                    on = "y+"
                if h == 0 and dy == 3 and e == 1:
                    on = "y-"
                if h == 1 and dx == 1 and e == 0:
                    on = "x+"
                if h == 1 and dx == 3 and e == 1:
                    on = "x-"
                plan[2 * i].append(((dy, dx), p, on))

    def step(t, carry):
        for when, events in plan.items():
            @pl.when(t == when)
            def _(events=events):
                for slot, p, on in events:
                    wait_a(slot, p)
                    if on:
                        send_a(slot, p, on)

        lrel = t // 2
        dy = jnp.where(lrel == 2, 3, jnp.where(lrel == 3, 2, lrel))
        ys = (yy + 4 - dy) % 4
        pair = (xx // 2 + t % 2) % 2
        unit = ys * 2 + pair
        slots = [dy * 4 + (xx + 4 - (2 * pair + o)) % 4 for o in range(2)]

        def outer(g, c2):
            lhs = bt[pl.ds(pl.multiple_of(2 * n192 * g, 128), 2 * n192), :]
            for o in range(2):
                rhs = jnp.concatenate(
                    [jnp.concatenate([a_buf[slots[o], p, 128 * q:128 * (q + 1), :] for q in range(3)], axis=1)
                     for p in range(NP)], axis=0)
                prod = dot(lhs, rhs)
                for q in range(3):
                    for h in range(2):
                        base = n192 * h
                        v = [prod[base + 48 * d:base + 48 * (d + 1), 128 * q:128 * (q + 1)] for d in range(4)]
                        for k, w in enumerate(transpose4(v)):
                            i = RES * o + 4 * q + k
                            lhs2[48 * i:48 * (i + 1), pl.ds(pl.multiple_of(256 * g + 128 * h, 128), 128)] = w.astype(BF16)
            return c2

        lax.fori_loop(0, 4, outer, 0)
        for c in range(3):
            res = dot(lhs2[384 * c:384 * (c + 1), :], wo_p[...])
            for k in range(8):
                i = 8 * c + k
                for jg in range(6):
                    rt[pl.ds(8 * jg * UNIT + i, 8, stride=UNIT), :] = res[48 * k + 8 * jg:48 * k + 8 * jg + 8, :]
        own = rt[0:RES * UNIT, :].astype(BF16)

        @pl.when(home == dap)
        def _():
            r_recv[zz % 2, dap, unit] = own

        for r in (2, 1, 3):
            r_send[t, r] = rt[RES * UNIT * r:RES * UNIT * (r + 1), :].astype(BF16)
            r_copy(t, r, unit).start()

        @pl.when(home != dap)
        def _():
            r_send[t, 0] = own
            r_copy(t, 0, unit).start()
        return carry

    lax.fori_loop(0, 8, step, 0)

    for dy in range(4):
        for dx in range(4):
            pos = ((yy + 4 - dy) % 4) * 4 + (xx + 4 - dx) % 4
            mask_all[pl.ds(pl.multiple_of(16 * pos, 16), 16), :] = jnp.concatenate(
                [a_buf[dy * 4 + dx, p, AROWS:PROWS, :] for p in range(NP)], axis=1)
    ro, co = iota((256, 256), 0), iota((256, 256), 1)
    squeeze = jnp.where((ro < 192) & ((ro // RES) * 16 + ro % RES == co), 1.0, 0.0).astype(BF16)
    mask_rows = dot(squeeze, mask_all[...]).astype(BF16)
    for r in range(4):
        mask_cols = jnp.concatenate([b_buf[r, p, AROWS:PROWS, :] for p in range(NP)], axis=1)
        part = dot(mask_cols, mask_rows, NT)
        if r:
            n_send[r] = part
            n_copy(r).start()
        else:
            @pl.when(home == dap)
            def _(part=part):
                n_recv[zz % 2, dap] = part

            @pl.when(home != dap)
            def _(part=part):
                n_send[0] = part
                n_copy(0).start()

    pltpu.make_async_copy(z_hbm, z_v, z_sem).wait()
    bo = bo_ref[...].astype(F32)

    def arrive(ref, sem, src):
        pltpu.make_async_remote_copy(
            src_ref=src, dst_ref=ref, send_sem=n_ss.at[0], recv_sem=sem,
            device_id=dev(col, other), device_id_type=MESH).wait_recv()

    for k in range(2):
        for c in range(2):
            @pl.when(jnp.logical_not((zz == 2 * dap + k) & (dap == c)))
            def _(k=k, c=c):
                arrive(n_recv.at[k, c], n_rs.at[k, c], n_send.at[0])
        inv = 1.0 / (1e-3 + (n_recv[k, 0] + n_recv[k, 1]))
        inv_v[k] = inv.T

    for k in range(2):
        def finish(u, carry, k=k):
            for c in range(2):
                @pl.when(jnp.logical_not((zz == 2 * dap + k) & (dap == c)))
                def _(c=c):
                    arrive(r_recv.at[k, c, u], r_rs.at[k, c, u], r_send.at[0, 0])
            rows = pl.ds(pl.multiple_of(UNIT * u, 8), UNIT)
            dst = pl.ds(pl.multiple_of(192 * k + UNIT * u, 8), UNIT)
            inv = inv_v[k, rows, :]
            total = r_recv[k, 0, u].astype(F32) + r_recv[k, 1, u].astype(F32) + bo
            for j in range(RES):
                out_v[j, dst, :] = z_v[j, dst, :] + total[UNIT * j:UNIT * (j + 1), :] * inv[:, j:j + 1]
            return carry

        lax.fori_loop(0, 8, finish, 0)
        half = pl.ds(192 * k, 192)
        pltpu.make_async_copy(out_v.at[:, half, :], out_hbm.at[:, half, :], o_sem.at[k]).start()

    for slot, p, way in a_sent:
        a_copy(slot, p, way).wait_send()
    for r, p, way in b_sent:
        b_copy(r, p, way).wait_send()

    def left(t, carry):
        for r in (1, 2, 3):
            r_copy(t, r, 0).wait_send()

        @pl.when(home != dap)
        def _():
            r_copy(t, 0, 0).wait_send()
        return carry

    lax.fori_loop(0, 8, left, 0)
    for r in (1, 2, 3):
        n_copy(r).wait_send()

    @pl.when(home != dap)
    def _():
        n_copy(0).wait_send()

    for k in range(2):
        half = pl.ds(192 * k, 192)
        pltpu.make_async_copy(out_v.at[:, half, :], out_hbm.at[:, half, :], o_sem.at[k]).wait()


def solution(mesh):
    row_spec = P(("data", "dap"), "col", None)
    mask_spec = P(("data", "dap"), "col")
    in_specs = (row_spec, mask_spec, row_spec) + (P(),) * 8
    any_spec = pl.BlockSpec(memory_space=pl.ANY)
    vmem = pl.BlockSpec(memory_space=pltpu.VMEM)
    dma = pltpu.SemaphoreType.DMA
    scratch = [
        pltpu.VMEM((NP, RES, PIECE, CH), BF16),
        pltpu.VMEM((16, SEQ), F32),
        pltpu.VMEM((128, 4 * CH), BF16),
        pltpu.VMEM((AROWS, PIECE), F32),
        pltpu.VMEM((16, NP, PROWS, 128), BF16),
        pltpu.VMEM((4, NP, PROWS, 128), BF16),
        pltpu.VMEM((4 * AROWS, SEQ), BF16),
        pltpu.VMEM((UNIT * 48, HID * HID), BF16),
        pltpu.VMEM((48 * UNIT, PAIR), F32),
        pltpu.VMEM((HID * HID, PAIR), F32),
        pltpu.VMEM((HID * HID, PAIR), BF16),
        pltpu.VMEM((8, 4, RES * UNIT, PAIR), BF16),
        pltpu.VMEM((2, 2, 8, RES * UNIT, PAIR), BF16),
        pltpu.VMEM((4, 16, 256), F32),
        pltpu.VMEM((2, 2, 16, 256), F32),
        pltpu.VMEM((256, SEQ), BF16),
        pltpu.VMEM((2, 256, 16), F32),
        pltpu.VMEM((RES, 384, PAIR), F32),
        pltpu.VMEM((RES, 384, PAIR), F32),
        dma((NP,)), dma, dma((2,)),
        dma((16, NP, 4)), dma((16, NP)), dma((4, NP, 2)), dma((4, NP)),
        dma((8, 4)), dma((2, 2, 8)), dma((4,)), dma((2, 2)),
    ]

    def local_fn(m, mask, z, gamma, beta, w_a, b_a, w_b, b_b, w_out, b_out):
        out = pl.pallas_call(
            kernel,
            out_shape=jax.ShapeDtypeStruct((RES, 384, PAIR), F32),
            in_specs=[any_spec, vmem, any_spec] + [vmem] * 8,
            out_specs=any_spec,
            scratch_shapes=scratch,
            compiler_params=pltpu.CompilerParams(
                collective_id=0, has_side_effects=True, vmem_limit_bytes=60 * 1024 * 1024),
            name="opm",
        )(jnp.transpose(m, (1, 0, 2)), mask.T, jnp.transpose(z, (1, 0, 2)), gamma.reshape(1, CH), beta.reshape(1, CH),
          w_a.T, b_a.reshape(1, HID), w_b.T, b_b.reshape(1, HID), w_out, b_out.reshape(1, PAIR))
        return jnp.transpose(out, (1, 0, 2))

    return jax.shard_map(local_fn, mesh=mesh, in_specs=in_specs, out_specs=row_spec, check_vma=False)
```

```python
import jax
import jax.numpy as jnp
from jax import lax
from jax.experimental import pallas as pl
from jax.experimental.pallas import tpu as pltpu
from jax.sharding import PartitionSpec as P

F32 = jnp.float32
BF16 = jnp.bfloat16
MESH = pl.DeviceIdType.MESH
NT = (((1,), (1,)), ((), ()))

SEQ, RES, CH, HID, PAIR = 512, 12, 256, 32, 128
PIECE = 128
NP = SEQ // PIECE
AROWS = RES * HID
PROWS = AROWS + 16
UNIT = 2 * RES

WAYS = ("x+", "x-", "y+", "y-", "z+", "z-")
MOVE = {"x+": (0, 0, 1), "x-": (0, 0, -1), "y+": (0, 1, 0), "y-": (0, -1, 0), "z+": (1, 0, 0), "z-": (-1, 0, 0)}
STEPS = ((0, 0), (0, 1), (1, 0), (3, 0), (3, 1), (1, 1), (2, 0), (2, 1))
THIRDS = 3


def onward(place, p):
    dz, dy, dx = place
    plus = p < 2

    def along(d, axis):
        return [axis + "+"] if d == 1 and plus else [axis + "-"] if d == 3 and not plus else []

    if dz:
        return along(dz, "z")
    first, second, d1, d2 = ("x", "y", dx, dy) if p % 2 == 0 else ("y", "x", dy, dx)
    if d2:
        return along(d2, second)
    return along(d1, first) + [second + "+", second + "-"]


def relay_order(piece=2.22, hop=2.3, out=2.37, start=3.0, norm=1.3, regroup=1.6, product=2.6, issue=0.05):
    link = dict.fromkeys(WAYS, 0.0)
    here, sent, order = {}, set(), {}
    now, at = 0.0, (-1, 0)

    def send(place, p, way):
        link[way] = max(link[way], now) + piece
        here[tuple((a + b) % 4 for a, b in zip(place, MOVE[way])), p] = link[way] + hop

    def relay():
        nonlocal now
        for (place, p), _ in sorted(((k, v) for k, v in here.items() if v <= now and k not in sent), key=lambda kv: kv[1]):
            sent.add((place, p))
            for way in onward(place, p):
                send(place, p, way)
                order.setdefault(at, []).append((place, p, way))
                now += issue

    def ready(blocks):
        return all(here.get((b, p), now + 1) <= now for b in blocks for p in range(NP) if any(b))

    for p in range(NP):
        now = start + norm * p
        for way in WAYS:
            send((0, 0, 0), p, way)
    now += norm / 3
    todo = [("b", [(d, 0, 0) for d in (1, 2, 3)])]
    todo += [(i, [(0, dy, 2 * far), (0, dy, 1 + 2 * far)]) for i, (dy, far) in enumerate(STEPS)]
    for what, blocks in todo:
        relay()
        while not ready(blocks):
            now = min(v for v in here.values() if v > now)
            relay()
        if what == "b":
            now += regroup
        else:
            for third in range(THIRDS):
                at = (what, third)
                relay()
                now += product / THIRDS
        at = (0 if what == "b" else what + 1, 0)
    return order


def iota(shape, axis):
    return lax.broadcasted_iota(jnp.int32, shape, axis)


def dot(a, b, dims=None):
    if dims is None:
        return jnp.dot(a, b, preferred_element_type=F32)
    return lax.dot_general(a, b, dims, preferred_element_type=F32)


def kernel(m_hbm, mask_ref, z_hbm, gamma_ref, beta_ref, wa_ref, ba_ref, wb_ref, bb_ref, wo_ref, bo_ref,
           out_ref,
           m_v, mask_v, wabig, b32, a_buf, b_buf, bt, lhs2, rt, w32, wo_p, r_send, r_recv, n_send, n_recv,
           mask_all, inv_v, z_v,
           m_sem, z_sem, a_ss, a_rs, b_ss, b_rs, r_ss, r_rs, n_ss, n_rs):
    col = lax.axis_index("col")
    dap = lax.axis_index("dap")
    zz, yy, xx = col // 16, (col // 4) % 4, col % 4
    home = zz // 2
    other = 1 - dap

    def at(dz=0, dy=0, dx=0):
        return ((zz + dz) % 4) * 16 + ((yy + dy) % 4) * 4 + (xx + dx) % 4

    def dev(c, d):
        return {"col": c, "dap": d}

    for p in range(NP):
        pltpu.make_async_copy(m_hbm.at[:, pl.ds(PIECE * p, PIECE), :], m_v.at[p], m_sem.at[p]).start()
    barrier = pltpu.get_barrier_semaphore()
    greet = [dev(at(dy=1), dap), dev(at(dy=3), dap), dev(at(dx=1), dap), dev(at(dx=3), dap), dev(col, other)]
    for r in (1, 2, 3):
        for d in (0, 1):
            greet.append(dev(at(dz=r), d))
    for who in greet:
        pl.semaphore_signal(barrier, inc=1, device_id=who, device_id_type=MESH)

    mask_v[...] = jnp.zeros_like(mask_v)
    mask_v[0:RES, :] = mask_ref[...].astype(F32)
    wa = wa_ref[...]
    for k in range(4):
        rows = [wa if kk == k else jnp.zeros_like(wa) for kk in range(4)]
        wabig[:, CH * k:CH * (k + 1)] = jnp.concatenate(rows, axis=0)
    gamma = gamma_ref[...].astype(F32).reshape(1, CH)
    beta = beta_ref[...].astype(F32).reshape(1, CH)
    tile4 = jnp.where(iota((HID, 128), 1) % HID == iota((HID, 128), 0), 1.0, 0.0).astype(BF16)
    ba_row = dot(jnp.broadcast_to(ba_ref[...], (16, HID)), tile4)[0:1, :]
    eye = iota((HID, HID), 0) == iota((HID, HID), 1)
    bb_diag = jnp.where(eye, jnp.broadcast_to(bb_ref[...], (HID, HID)).astype(F32), 0.0).astype(BF16)
    bb_col = dot(bb_diag, jnp.ones((HID, 128), BF16))

    def hop(place, p, way):
        to = tuple((d + s) % 4 for d, s in zip(place, MOVE[way]))
        w = WAYS.index(way) % 4 % 2 + 2 * (way[0] == "y")
        if way[0] == "z":
            return pltpu.make_async_remote_copy(
                src_ref=b_buf.at[place[0], p], dst_ref=b_buf.at[to[0], p], send_sem=b_ss.at[place[0], p, w],
                recv_sem=b_rs.at[to[0], p], device_id=dev(at(*MOVE[way]), dap), device_id_type=MESH)
        src, dst = place[1] * 4 + place[2], to[1] * 4 + to[2]
        return pltpu.make_async_remote_copy(
            src_ref=a_buf.at[src, p], dst_ref=a_buf.at[dst, p], send_sem=a_ss.at[src, p, w],
            recv_sem=a_rs.at[dst, p], device_id=dev(at(*MOVE[way]), dap), device_id_type=MESH)

    def wait_a(i, p):
        pltpu.make_async_remote_copy(
            src_ref=a_buf.at[i, p], dst_ref=a_buf.at[i, p], send_sem=a_ss.at[i, p, 0], recv_sem=a_rs.at[i, p],
            device_id=dev(at(dx=1), dap), device_id_type=MESH).wait_recv()

    def wait_b(r, p):
        pltpu.make_async_remote_copy(
            src_ref=b_buf.at[r, p], dst_ref=b_buf.at[r, p], send_sem=b_ss.at[r, p, 0], recv_sem=b_rs.at[r, p],
            device_id=dev(at(dz=1), dap), device_id_type=MESH).wait_recv()

    hops = relay_order()
    sent = [((0, 0, 0), p, way) for p in range(NP) for way in WAYS]
    seen = set()

    def run(key):
        for place, p, way in hops.get(key, ()):
            if (place, p) not in seen:
                seen.add((place, p))
                if place[0]:
                    wait_b(place[0], p)
                else:
                    wait_a(place[1] * 4 + place[2], p)
            hop(place, p, way).start()
            sent.append((place, p, way))

    def project(p, carry):
        pltpu.make_async_copy(m_hbm.at[:, pl.ds(0, PIECE), :], m_v.at[p], m_sem.at[p]).wait()
        lanes = pl.ds(pl.multiple_of(PIECE * p, PIECE), PIECE)
        mask_p = mask_v[:, lanes]
        mask_b = mask_p.astype(BF16)
        mask_t = mask_p.T.astype(BF16)
        for q in range(3):
            xs = []
            for k in range(4):
                n = 4 * q + k
                v = m_v[p, n].astype(F32)
                mean = jnp.sum(v, axis=1, keepdims=True) * (1.0 / CH)
                cen = v - mean
                var = jnp.sum(cen * cen, axis=1, keepdims=True) * (1.0 / CH)
                x = (cen * lax.rsqrt(var + 1e-5) * gamma + beta).astype(BF16)
                xs.append(x)
                lin_b = dot(wb_ref[...], x, NT)
                b32[pl.ds(n, HID, stride=RES), :] = (lin_b + bb_col) * mask_p[n:n + 1, :]
            lin_a = dot(jnp.concatenate(xs, axis=1), wabig[...], NT)
            spread = jnp.where(iota((16, 128), 1) // HID + 4 * q == iota((16, 128), 0), 1.0, 0.0).astype(BF16)
            a_buf[0, p, 128 * q:128 * (q + 1), :] = ((lin_a + ba_row) * dot(mask_t, spread)).astype(BF16)
        a_buf[0, p, AROWS:PROWS, :] = mask_b
        b_buf[0, p, 0:AROWS, :] = b32[...].astype(BF16)
        b_buf[0, p, AROWS:PROWS, :] = mask_b

        @pl.when(p == 0)
        def _():
            pl.semaphore_wait(barrier, len(greet))

        for way in WAYS[4:] + WAYS[:4]:
            hop((0, 0, 0), p, way).start()
        return carry

    lax.fori_loop(0, NP, project, 0)
    pltpu.make_async_copy(z_hbm, z_v, z_sem).start()

    w32[...] = wo_ref[...].astype(F32)

    def order(d, carry):
        wo_p[pl.ds(pl.multiple_of(HID * d, HID), HID), :] = w32[pl.ds(d, HID, stride=HID), :].astype(BF16)
        return carry

    lax.fori_loop(0, HID, order, 0)

    run((-1, 0))

    for r in (1, 3, 2):
        for p in range(NP):
            if ((r, 0, 0), p) not in seen:
                wait_b(r, p)
    n192 = 4 * 4 * RES
    ro, co = iota((n192, n192), 0), iota((n192, n192), 1)
    want = ((ro // RES) % 4) * 48 + (ro // 48) * RES + ro % RES
    perm = jnp.where(want == co, 1.0, 0.0).astype(BF16)

    def regroup(g, carry):
        rows = pl.ds(pl.multiple_of(48 * g, 16), 48)
        cat = jnp.concatenate(
            [jnp.concatenate([b_buf[r, p, rows, :] for p in range(NP)], axis=1) for r in range(4)], axis=0)
        bt[pl.ds(pl.multiple_of(n192 * g, 64), n192), :] = dot(perm, cat).astype(BF16)
        return carry

    lax.fori_loop(0, 8, regroup, 0)

    lane = iota((1, 128), 1)
    low = lane < 64
    odd = (lane // HID) % 2 == 1

    def transpose4(v):
        def swap(u, w):
            t = pltpu.roll(jnp.where(low, w, u), 64, 1)
            return jnp.where(low, u, t), jnp.where(low, t, w)

        def swap2(u, w):
            return (jnp.where(odd, pltpu.roll(w, 32, 1), u), jnp.where(odd, w, pltpu.roll(u, 96, 1)))

        e0, e2 = swap(v[0], v[2])
        e1, e3 = swap(v[1], v[3])
        w0, w1 = swap2(e0, e1)
        w2, w3 = swap2(e2, e3)
        return w0, w1, w2, w3

    def r_copy(t, r, unit):
        return pltpu.make_async_remote_copy(
            src_ref=r_send.at[t, r], dst_ref=r_recv.at[zz % 2, dap, unit], send_sem=r_ss.at[t, r],
            recv_sem=r_rs.at[zz % 2, dap, unit], device_id=dev(at(dz=-r), home), device_id_type=MESH)

    def n_copy(r):
        return pltpu.make_async_remote_copy(
            src_ref=n_send.at[r], dst_ref=n_recv.at[zz % 2, dap], send_sem=n_ss.at[r],
            recv_sem=n_rs.at[zz % 2, dap], device_id=dev(at(dz=-r), home), device_id_type=MESH)

    def count():
        for dy in range(4):
            for dx in range(4):
                pos = ((yy + 4 - dy) % 4) * 4 + (xx + 4 - dx) % 4
                mask_all[pl.ds(pl.multiple_of(16 * pos, 16), 16), :] = jnp.concatenate(
                    [a_buf[dy * 4 + dx, p, AROWS:PROWS, :] for p in range(NP)], axis=1)
        ro, co = iota((256, 256), 0), iota((256, 256), 1)
        squeeze = jnp.where((ro < 192) & ((ro // RES) * 16 + ro % RES == co), 1.0, 0.0).astype(BF16)
        mask_rows = dot(squeeze, mask_all[...]).astype(BF16)
        for r in range(4):
            mask_cols = jnp.concatenate([b_buf[r, p, AROWS:PROWS, :] for p in range(NP)], axis=1)
            part = dot(mask_cols, mask_rows, NT)
            if r:
                n_send[r] = part
                n_copy(r).start()
            else:
                @pl.when(home == dap)
                def _(part=part):
                    n_recv[zz % 2, dap] = part

                @pl.when(home != dap)
                def _(part=part):
                    n_send[0] = part
                    n_copy(0).start()

    rest = {0: (), 1: (2,), 3: (0,), 2: (0, 2)}
    px = 3 - 2 * (xx % 2)

    def place(t):
        dy, far = jnp.int32(STEPS[7][0]), jnp.int32(STEPS[7][1])
        for i in range(6, -1, -1):
            dy = jnp.where(t == i, STEPS[i][0], dy)
            far = jnp.where(t == i, STEPS[i][1], far)
        pair = (xx // 2 + far) % 2
        return dy, pair, ((yy + 4 - dy) % 4) * 2 + pair

    def step(t, carry):
        for at_t in range(8):
            @pl.when(t == at_t)
            def _(at_t=at_t):
                run((at_t, 0))
                dy, far = STEPS[at_t]
                if not far:
                    for p in rest[dy]:
                        wait_a(dy * 4, p)
                    near, p = dy * 4 + px, 4 - px
                else:
                    for p in rest[dy] + (1, 3):
                        wait_a(dy * 4 + 2, p)
                    near, p = dy * 4 + 4 - px, px
                for q in rest[dy]:
                    wait_a(near, q)
                wait_a(near, p)
                if at_t == 7:
                    count()

        dy, pair, unit = place(t)
        slots = [dy * 4 + (xx + 4 - (2 * pair + o)) % 4 for o in range(2)]

        for c in range(THIRDS):
            for at_t in range(8):
                if c and (at_t, c) in hops:
                    @pl.when(t == at_t)
                    def _(at_t=at_t, c=c):
                        run((at_t, c))
            quads = (2 * c, 2 * c + 1)
            rhs = jnp.concatenate(
                [jnp.concatenate([a_buf[slots[q // 3], p, 128 * (q % 3):128 * (q % 3 + 1), :] for q in quads], axis=1)
                 for p in range(NP)], axis=0)
            for g in range(2):
                prod = dot(bt[4 * n192 * g:4 * n192 * (g + 1), :], rhs)
                for h in range(4):
                    for k2, q in enumerate(quads):
                        base = n192 * h
                        v = [prod[base + 48 * d:base + 48 * (d + 1), 128 * k2:128 * (k2 + 1)] for d in range(4)]
                        for k, w in enumerate(transpose4(v)):
                            i = 4 * q + k
                            lhs2[4 * g + h, 48 * i:48 * (i + 1), :] = w.astype(BF16)
        res = dot(jnp.concatenate([lhs2[g] for g in range(8)], axis=1), wo_p[...])
        for i in range(UNIT):
            for jg in range(6):
                rt[pl.ds(8 * jg * UNIT + i, 8, stride=UNIT), :] = res[48 * i + 8 * jg:48 * i + 8 * jg + 8, :]
        own = rt[0:RES * UNIT, :].astype(BF16)

        @pl.when(home == dap)
        def _():
            r_recv[zz % 2, dap, unit] = own

        for r in (2, 1, 3):
            r_send[t, r] = rt[RES * UNIT * r:RES * UNIT * (r + 1), :].astype(BF16)
            r_copy(t, r, unit).start()

        @pl.when(home != dap)
        def _():
            r_send[t, 0] = own
            r_copy(t, 0, unit).start()
        return carry

    lax.fori_loop(0, 8, step, 0)

    pltpu.make_async_copy(z_hbm, z_v, z_sem).wait()
    bo = bo_ref[...].astype(F32)

    def arrive(ref, sem, src):
        pltpu.make_async_remote_copy(
            src_ref=src, dst_ref=ref, send_sem=n_ss.at[0], recv_sem=sem,
            device_id=dev(col, other), device_id_type=MESH).wait_recv()

    for k in range(2):
        for c in range(2):
            @pl.when(jnp.logical_not((zz == 2 * dap + k) & (dap == c)))
            def _(k=k, c=c):
                arrive(n_recv.at[k, c], n_rs.at[k, c], n_send.at[0])
        inv = 1.0 / (1e-3 + (n_recv[k, 0] + n_recv[k, 1]))
        inv_v[k] = inv.T

    def finish(t, carry):
        _, _, u = place(t)
        for k in range(2):
            for c in range(2):
                @pl.when(jnp.logical_not((zz == 2 * dap + k) & (dap == c)))
                def _(k=k, c=c):
                    arrive(r_recv.at[k, c, u], r_rs.at[k, c, u], r_send.at[0, 0])
            rows = pl.ds(pl.multiple_of(UNIT * u, 8), UNIT)
            dst = pl.ds(pl.multiple_of(192 * k + UNIT * u, 8), UNIT)
            inv = inv_v[k, rows, :]
            total = r_recv[k, 0, u].astype(F32) + r_recv[k, 1, u].astype(F32) + bo
            for j in range(RES):
                out_ref[j, dst, :] = z_v[j, dst, :] + total[UNIT * j:UNIT * (j + 1), :] * inv[:, j:j + 1]
        return carry

    lax.fori_loop(0, 8, finish, 0)

    for place, p, way in sent:
        hop(place, p, way).wait_send()

    def left(t, carry):
        for r in (1, 2, 3):
            r_copy(t, r, 0).wait_send()

        @pl.when(home != dap)
        def _():
            r_copy(t, 0, 0).wait_send()
        return carry

    lax.fori_loop(0, 8, left, 0)
    for r in (1, 2, 3):
        n_copy(r).wait_send()

    @pl.when(home != dap)
    def _():
        n_copy(0).wait_send()


def solution(mesh):
    row_spec = P(("data", "dap"), "col", None)
    mask_spec = P(("data", "dap"), "col")
    in_specs = (row_spec, mask_spec, row_spec) + (P(),) * 8
    any_spec = pl.BlockSpec(memory_space=pl.ANY)
    vmem = pl.BlockSpec(memory_space=pltpu.VMEM)
    dma = pltpu.SemaphoreType.DMA
    scratch = [
        pltpu.VMEM((NP, RES, PIECE, CH), BF16),
        pltpu.VMEM((16, SEQ), F32),
        pltpu.VMEM((128, 4 * CH), BF16),
        pltpu.VMEM((AROWS, PIECE), F32),
        pltpu.VMEM((16, NP, PROWS, 128), BF16),
        pltpu.VMEM((4, NP, PROWS, 128), BF16),
        pltpu.VMEM((4 * AROWS, SEQ), BF16),
        pltpu.VMEM((8, UNIT * 48, 128), BF16),
        pltpu.VMEM((48 * UNIT, PAIR), F32),
        pltpu.VMEM((HID * HID, PAIR), F32),
        pltpu.VMEM((HID * HID, PAIR), BF16),
        pltpu.VMEM((8, 4, RES * UNIT, PAIR), BF16),
        pltpu.VMEM((2, 2, 8, RES * UNIT, PAIR), BF16),
        pltpu.VMEM((4, 16, 256), F32),
        pltpu.VMEM((2, 2, 16, 256), F32),
        pltpu.VMEM((256, SEQ), BF16),
        pltpu.VMEM((2, 256, 16), F32),
        pltpu.VMEM((RES, 384, PAIR), F32),
        dma((NP,)), dma,
        dma((16, NP, 4)), dma((16, NP)), dma((4, NP, 2)), dma((4, NP)),
        dma((8, 4)), dma((2, 2, 8)), dma((4,)), dma((2, 2)),
    ]

    def local_fn(m, mask, z, gamma, beta, w_a, b_a, w_b, b_b, w_out, b_out):
        out = pl.pallas_call(
            kernel,
            out_shape=pltpu.VMEM((RES, 384, PAIR), F32),
            in_specs=[any_spec, vmem, any_spec] + [vmem] * 8,
            out_specs=vmem,
            scratch_shapes=scratch,
            compiler_params=pltpu.CompilerParams(
                collective_id=0, has_side_effects=True, vmem_limit_bytes=60 * 1024 * 1024),
            name="opm",
        )(jnp.transpose(m, (1, 0, 2)), mask.T, jnp.transpose(z, (1, 0, 2)), gamma, beta,
          w_a.T, b_a.reshape(1, HID), w_b.T, b_b.reshape(1, HID), w_out, b_out.reshape(1, PAIR))
        return jnp.transpose(out, (1, 0, 2))

    return jax.shard_map(local_fn, mesh=mesh, in_specs=in_specs, out_specs=row_spec, check_vma=False)
```

```python
import jax
import jax.numpy as jnp
from jax import lax
from jax.experimental import pallas as pl
from jax.experimental.pallas import tpu as pltpu
from jax.sharding import PartitionSpec as P

F32 = jnp.float32
BF16 = jnp.bfloat16
MESH = pl.DeviceIdType.MESH
NT = (((1,), (1,)), ((), ()))

SEQ, RES, CH, HID, PAIR = 512, 12, 256, 32, 128
PIECE = 128
NP = SEQ // PIECE
AROWS = RES * HID
PROWS = AROWS + 16
UNIT = 2 * RES

WAYS = ("x+", "x-", "y+", "y-", "z+", "z-")
MOVE = {"x+": (0, 0, 1), "x-": (0, 0, -1), "y+": (0, 1, 0), "y-": (0, -1, 0), "z+": (1, 0, 0), "z-": (-1, 0, 0)}
STEPS = ((0, 0), (0, 1), (1, 0), (3, 0), (3, 1), (1, 1), (2, 0), (2, 1))


def onward(place, p):
    dz, dy, dx = place
    plus = p < 2

    def along(d, axis):
        return [axis + "+"] if d == 1 and plus else [axis + "-"] if d == 3 and not plus else []

    if dz:
        return along(dz, "z")
    first, second, d1, d2 = ("x", "y", dx, dy) if p % 2 == 0 else ("y", "x", dy, dx)
    if d2:
        return along(d2, second)
    return along(d1, first) + [second + "+", second + "-"]


def relay_order(piece=2.22, hop=2.3, out=2.37, start=3.0, norm=1.3, regroup=1.6, product=2.6, issue=0.05):
    link = dict.fromkeys(WAYS, 0.0)
    here, sent, order = {}, set(), {}
    now, at = 0.0, -1

    def send(place, p, way):
        link[way] = max(link[way], now) + piece
        here[tuple((a + b) % 4 for a, b in zip(place, MOVE[way])), p] = link[way] + hop

    def relay():
        nonlocal now
        for (place, p), _ in sorted(((k, v) for k, v in here.items() if v <= now and k not in sent), key=lambda kv: kv[1]):
            sent.add((place, p))
            for way in onward(place, p):
                send(place, p, way)
                order.setdefault(at, []).append((place, p, way))
                now += issue

    def ready(blocks):
        return all(here.get((b, p), now + 1) <= now for b in blocks for p in range(NP) if any(b))

    for p in range(NP):
        now = start + norm * p
        for way in WAYS:
            send((0, 0, 0), p, way)
    now += norm / 3
    todo = [("b", [(d, 0, 0) for d in (1, 2, 3)])]
    todo += [(i, [(0, dy, 2 * far), (0, dy, 1 + 2 * far)]) for i, (dy, far) in enumerate(STEPS)]
    for what, blocks in todo:
        relay()
        while not ready(blocks):
            now = min(v for v in here.values() if v > now)
            relay()
        if what == "b":
            now += regroup
        else:
            now += product
        at = 0 if what == "b" else what + 1
    return order


def iota(shape, axis):
    return lax.broadcasted_iota(jnp.int32, shape, axis)


def dot(a, b, dims=None):
    if dims is None:
        return jnp.dot(a, b, preferred_element_type=F32)
    return lax.dot_general(a, b, dims, preferred_element_type=F32)


def kernel(m_hbm, mask_ref, z_hbm, gamma_ref, beta_ref, wa_ref, ba_ref, wb_ref, bb_ref, wo_ref, bo_ref,
           out_ref,
           m_v, mask_v, wabig, b32, a_buf, b_buf, bt, lhs2, rt, w32, wo_p, r_send, r_recv, n_send, n_recv,
           mask_all, inv_v, z_v,
           m_sem, z_sem, a_ss, a_rs, b_ss, b_rs, r_ss, r_rs, n_ss, n_rs):
    col = lax.axis_index("col")
    dap = lax.axis_index("dap")
    zz, yy, xx = col // 16, (col // 4) % 4, col % 4
    home = zz // 2
    other = 1 - dap

    def at(dz=0, dy=0, dx=0):
        return ((zz + dz) % 4) * 16 + ((yy + dy) % 4) * 4 + (xx + dx) % 4

    def dev(c, d):
        return {"col": c, "dap": d}

    for p in range(NP):
        pltpu.make_async_copy(m_hbm.at[:, pl.ds(PIECE * p, PIECE), :], m_v.at[p], m_sem.at[p]).start()
    barrier = pltpu.get_barrier_semaphore()
    greet = [dev(at(dy=1), dap), dev(at(dy=3), dap), dev(at(dx=1), dap), dev(at(dx=3), dap), dev(col, other)]
    for r in (1, 2, 3):
        for d in (0, 1):
            greet.append(dev(at(dz=r), d))
    for who in greet:
        pl.semaphore_signal(barrier, inc=1, device_id=who, device_id_type=MESH)

    mask_v[...] = jnp.zeros_like(mask_v)
    mask_v[0:RES, :] = mask_ref[...].astype(F32)
    wa = wa_ref[...]
    for k in range(4):
        rows = [wa if kk == k else jnp.zeros_like(wa) for kk in range(4)]
        wabig[:, CH * k:CH * (k + 1)] = jnp.concatenate(rows, axis=0)
    gamma = gamma_ref[...].astype(F32).reshape(1, CH)
    beta = beta_ref[...].astype(F32).reshape(1, CH)
    tile4 = jnp.where(iota((HID, 128), 1) % HID == iota((HID, 128), 0), 1.0, 0.0).astype(BF16)
    ba_row = dot(jnp.broadcast_to(ba_ref[...], (16, HID)), tile4)[0:1, :]
    eye = iota((HID, HID), 0) == iota((HID, HID), 1)
    bb_diag = jnp.where(eye, jnp.broadcast_to(bb_ref[...], (HID, HID)).astype(F32), 0.0).astype(BF16)
    bb_col = dot(bb_diag, jnp.ones((HID, 128), BF16))

    def hop(place, p, way):
        to = tuple((d + s) % 4 for d, s in zip(place, MOVE[way]))
        w = WAYS.index(way) % 4 % 2 + 2 * (way[0] == "y")
        if way[0] == "z":
            return pltpu.make_async_remote_copy(
                src_ref=b_buf.at[place[0], p], dst_ref=b_buf.at[to[0], p], send_sem=b_ss.at[place[0], p, w],
                recv_sem=b_rs.at[to[0], p], device_id=dev(at(*MOVE[way]), dap), device_id_type=MESH)
        src, dst = place[1] * 4 + place[2], to[1] * 4 + to[2]
        return pltpu.make_async_remote_copy(
            src_ref=a_buf.at[src, p], dst_ref=a_buf.at[dst, p], send_sem=a_ss.at[src, p, w],
            recv_sem=a_rs.at[dst, p], device_id=dev(at(*MOVE[way]), dap), device_id_type=MESH)

    def wait_a(i, p):
        pltpu.make_async_remote_copy(
            src_ref=a_buf.at[i, p], dst_ref=a_buf.at[i, p], send_sem=a_ss.at[i, p, 0], recv_sem=a_rs.at[i, p],
            device_id=dev(at(dx=1), dap), device_id_type=MESH).wait_recv()

    def wait_b(r, p):
        pltpu.make_async_remote_copy(
            src_ref=b_buf.at[r, p], dst_ref=b_buf.at[r, p], send_sem=b_ss.at[r, p, 0], recv_sem=b_rs.at[r, p],
            device_id=dev(at(dz=1), dap), device_id_type=MESH).wait_recv()

    hops = relay_order()
    sent = [((0, 0, 0), p, way) for p in range(NP) for way in WAYS]
    seen = set()

    def run(key):
        for place, p, way in hops.get(key, ()):
            if (place, p) not in seen:
                seen.add((place, p))
                if place[0]:
                    wait_b(place[0], p)
                else:
                    wait_a(place[1] * 4 + place[2], p)
            hop(place, p, way).start()
            sent.append((place, p, way))

    def project(p, carry):
        pltpu.make_async_copy(m_hbm.at[:, pl.ds(0, PIECE), :], m_v.at[p], m_sem.at[p]).wait()
        lanes = pl.ds(pl.multiple_of(PIECE * p, PIECE), PIECE)
        mask_p = mask_v[:, lanes]
        mask_b = mask_p.astype(BF16)
        mask_t = mask_p.T.astype(BF16)
        for q in range(3):
            xs = []
            for k in range(4):
                n = 4 * q + k
                v = m_v[p, n].astype(F32)
                mean = jnp.sum(v, axis=1, keepdims=True) * (1.0 / CH)
                cen = v - mean
                var = jnp.sum(cen * cen, axis=1, keepdims=True) * (1.0 / CH)
                x = (cen * lax.rsqrt(var + 1e-5) * gamma + beta).astype(BF16)
                xs.append(x)
                lin_b = dot(wb_ref[...], x, NT)
                b32[pl.ds(n, HID, stride=RES), :] = (lin_b + bb_col) * mask_p[n:n + 1, :]
            lin_a = dot(jnp.concatenate(xs, axis=1), wabig[...], NT)
            spread = jnp.where(iota((16, 128), 1) // HID + 4 * q == iota((16, 128), 0), 1.0, 0.0).astype(BF16)
            a_buf[0, p, 128 * q:128 * (q + 1), :] = ((lin_a + ba_row) * dot(mask_t, spread)).astype(BF16)
        a_buf[0, p, AROWS:PROWS, :] = mask_b
        b_buf[0, p, 0:AROWS, :] = b32[...].astype(BF16)
        b_buf[0, p, AROWS:PROWS, :] = mask_b

        @pl.when(p == 0)
        def _():
            pl.semaphore_wait(barrier, len(greet))

        for way in WAYS[4:] + WAYS[:4]:
            hop((0, 0, 0), p, way).start()
        return carry

    lax.fori_loop(0, NP, project, 0)
    pltpu.make_async_copy(z_hbm, z_v, z_sem).start()

    w32[...] = wo_ref[...].astype(F32)

    def order(d, carry):
        wo_p[pl.ds(pl.multiple_of(HID * d, HID), HID), :] = w32[pl.ds(d, HID, stride=HID), :].astype(BF16)
        return carry

    lax.fori_loop(0, HID, order, 0)

    run(-1)

    for r in (1, 3, 2):
        for p in range(NP):
            if ((r, 0, 0), p) not in seen:
                wait_b(r, p)
    n192 = 4 * 4 * RES
    ro, co = iota((n192, n192), 0), iota((n192, n192), 1)
    want = ((ro // RES) % 4) * 48 + (ro // 48) * RES + ro % RES
    perm = jnp.where(want == co, 1.0, 0.0).astype(BF16)

    def regroup(g, carry):
        rows = pl.ds(pl.multiple_of(48 * g, 16), 48)
        cat = jnp.concatenate(
            [jnp.concatenate([b_buf[r, p, rows, :] for p in range(NP)], axis=1) for r in range(4)], axis=0)
        bt[pl.ds(pl.multiple_of(n192 * g, 64), n192), :] = dot(perm, cat).astype(BF16)
        return carry

    lax.fori_loop(0, 8, regroup, 0)

    lane = iota((1, 128), 1)
    low = lane < 64
    odd = (lane // HID) % 2 == 1

    def transpose4(v):
        def swap(u, w):
            t = pltpu.roll(jnp.where(low, w, u), 64, 1)
            return jnp.where(low, u, t), jnp.where(low, t, w)

        def swap2(u, w):
            return (jnp.where(odd, pltpu.roll(w, 32, 1), u), jnp.where(odd, w, pltpu.roll(u, 96, 1)))

        e0, e2 = swap(v[0], v[2])
        e1, e3 = swap(v[1], v[3])
        w0, w1 = swap2(e0, e1)
        w2, w3 = swap2(e2, e3)
        return w0, w1, w2, w3

    def r_copy(t, r, unit):
        return pltpu.make_async_remote_copy(
            src_ref=r_send.at[t, r], dst_ref=r_recv.at[zz % 2, dap, unit], send_sem=r_ss.at[t, r],
            recv_sem=r_rs.at[zz % 2, dap, unit], device_id=dev(at(dz=-r), home), device_id_type=MESH)

    def n_copy(r):
        return pltpu.make_async_remote_copy(
            src_ref=n_send.at[r], dst_ref=n_recv.at[zz % 2, dap], send_sem=n_ss.at[r],
            recv_sem=n_rs.at[zz % 2, dap], device_id=dev(at(dz=-r), home), device_id_type=MESH)

    def count():
        for dy in range(4):
            for dx in range(4):
                pos = ((yy + 4 - dy) % 4) * 4 + (xx + 4 - dx) % 4
                mask_all[pl.ds(pl.multiple_of(16 * pos, 16), 16), :] = jnp.concatenate(
                    [a_buf[dy * 4 + dx, p, AROWS:PROWS, :] for p in range(NP)], axis=1)
        ro, co = iota((256, 256), 0), iota((256, 256), 1)
        squeeze = jnp.where((ro < 192) & ((ro // RES) * 16 + ro % RES == co), 1.0, 0.0).astype(BF16)
        mask_rows = dot(squeeze, mask_all[...]).astype(BF16)
        for r in range(4):
            mask_cols = jnp.concatenate([b_buf[r, p, AROWS:PROWS, :] for p in range(NP)], axis=1)
            part = dot(mask_cols, mask_rows, NT)
            if r:
                n_send[r] = part
                n_copy(r).start()
            else:
                @pl.when(home == dap)
                def _(part=part):
                    n_recv[zz % 2, dap] = part

                @pl.when(home != dap)
                def _(part=part):
                    n_send[0] = part
                    n_copy(0).start()

    rest = {0: (), 1: (2,), 3: (0,), 2: (0, 2)}
    px = 3 - 2 * (xx % 2)

    def place(t):
        dy, far = jnp.int32(STEPS[7][0]), jnp.int32(STEPS[7][1])
        for i in range(6, -1, -1):
            dy = jnp.where(t == i, STEPS[i][0], dy)
            far = jnp.where(t == i, STEPS[i][1], far)
        pair = (xx // 2 + far) % 2
        return dy, pair, ((yy + 4 - dy) % 4) * 2 + pair

    def step(t, carry):
        for at_t in range(8):
            @pl.when(t == at_t)
            def _(at_t=at_t):
                run(at_t)
                dy, far = STEPS[at_t]
                if not far:
                    for p in rest[dy]:
                        wait_a(dy * 4, p)
                    near, p = dy * 4 + px, 4 - px
                else:
                    for p in rest[dy] + (1, 3):
                        wait_a(dy * 4 + 2, p)
                    near, p = dy * 4 + 4 - px, px
                for q in rest[dy]:
                    wait_a(near, q)
                wait_a(near, p)
                if at_t == 7:
                    count()

        dy, pair, unit = place(t)
        slots = [dy * 4 + (xx + 4 - (2 * pair + o)) % 4 for o in range(2)]

        for c in range(3):
            quads = (2 * c, 2 * c + 1)
            rhs = jnp.concatenate(
                [jnp.concatenate([a_buf[slots[q // 3], p, 128 * (q % 3):128 * (q % 3 + 1), :] for q in quads], axis=1)
                 for p in range(NP)], axis=0)
            for g in range(2):
                prod = dot(bt[4 * n192 * g:4 * n192 * (g + 1), :], rhs)
                for h in range(4):
                    for k2, q in enumerate(quads):
                        base = n192 * h
                        v = [prod[base + 48 * d:base + 48 * (d + 1), 128 * k2:128 * (k2 + 1)] for d in range(4)]
                        for k, w in enumerate(transpose4(v)):
                            i = 4 * q + k
                            lhs2[4 * g + h, 48 * i:48 * (i + 1), :] = w.astype(BF16)
        res = dot(jnp.concatenate([lhs2[g] for g in range(8)], axis=1), wo_p[...])
        for i in range(UNIT):
            for jg in range(6):
                rt[pl.ds(8 * jg * UNIT + i, 8, stride=UNIT), :] = res[48 * i + 8 * jg:48 * i + 8 * jg + 8, :]
        own = rt[0:RES * UNIT, :].astype(BF16)

        @pl.when(home == dap)
        def _():
            r_recv[zz % 2, dap, unit] = own

        for r in (2, 1, 3):
            r_send[t, r] = rt[RES * UNIT * r:RES * UNIT * (r + 1), :].astype(BF16)
            r_copy(t, r, unit).start()

        @pl.when(home != dap)
        def _():
            r_send[t, 0] = own
            r_copy(t, 0, unit).start()
        return carry

    lax.fori_loop(0, 8, step, 0)

    pltpu.make_async_copy(z_hbm, z_v, z_sem).wait()
    bo = bo_ref[...].astype(F32)

    def arrive(ref, sem, src):
        pltpu.make_async_remote_copy(
            src_ref=src, dst_ref=ref, send_sem=n_ss.at[0], recv_sem=sem,
            device_id=dev(col, other), device_id_type=MESH).wait_recv()

    for k in range(2):
        for c in range(2):
            @pl.when(jnp.logical_not((zz == 2 * dap + k) & (dap == c)))
            def _(k=k, c=c):
                arrive(n_recv.at[k, c], n_rs.at[k, c], n_send.at[0])
        inv = 1.0 / (1e-3 + (n_recv[k, 0] + n_recv[k, 1]))
        inv_v[k] = inv.T

    def finish(t, carry):
        _, _, u = place(t)
        for k in range(2):
            for c in range(2):
                @pl.when(jnp.logical_not((zz == 2 * dap + k) & (dap == c)))
                def _(k=k, c=c):
                    arrive(r_recv.at[k, c, u], r_rs.at[k, c, u], r_send.at[0, 0])
            rows = pl.ds(pl.multiple_of(UNIT * u, 8), UNIT)
            dst = pl.ds(pl.multiple_of(192 * k + UNIT * u, 8), UNIT)
            inv = inv_v[k, rows, :]
            total = r_recv[k, 0, u].astype(F32) + r_recv[k, 1, u].astype(F32) + bo
            for j in range(RES):
                out_ref[j, dst, :] = z_v[j, dst, :] + total[UNIT * j:UNIT * (j + 1), :] * inv[:, j:j + 1]
        return carry

    lax.fori_loop(0, 8, finish, 0)

    for place, p, way in sent:
        hop(place, p, way).wait_send()

    def left(t, carry):
        for r in (1, 2, 3):
            r_copy(t, r, 0).wait_send()

        @pl.when(home != dap)
        def _():
            r_copy(t, 0, 0).wait_send()
        return carry

    lax.fori_loop(0, 8, left, 0)
    for r in (1, 2, 3):
        n_copy(r).wait_send()

    @pl.when(home != dap)
    def _():
        n_copy(0).wait_send()


def solution(mesh):
    row_spec = P(("data", "dap"), "col", None)
    mask_spec = P(("data", "dap"), "col")
    in_specs = (row_spec, mask_spec, row_spec) + (P(),) * 8
    any_spec = pl.BlockSpec(memory_space=pl.ANY)
    vmem = pl.BlockSpec(memory_space=pltpu.VMEM)
    dma = pltpu.SemaphoreType.DMA
    scratch = [
        pltpu.VMEM((NP, RES, PIECE, CH), BF16),
        pltpu.VMEM((16, SEQ), F32),
        pltpu.VMEM((128, 4 * CH), BF16),
        pltpu.VMEM((AROWS, PIECE), F32),
        pltpu.VMEM((16, NP, PROWS, 128), BF16),
        pltpu.VMEM((4, NP, PROWS, 128), BF16),
        pltpu.VMEM((4 * AROWS, SEQ), BF16),
        pltpu.VMEM((8, UNIT * 48, 128), BF16),
        pltpu.VMEM((48 * UNIT, PAIR), F32),
        pltpu.VMEM((HID * HID, PAIR), F32),
        pltpu.VMEM((HID * HID, PAIR), BF16),
        pltpu.VMEM((8, 4, RES * UNIT, PAIR), BF16),
        pltpu.VMEM((2, 2, 8, RES * UNIT, PAIR), BF16),
        pltpu.VMEM((4, 16, 256), F32),
        pltpu.VMEM((2, 2, 16, 256), F32),
        pltpu.VMEM((256, SEQ), BF16),
        pltpu.VMEM((2, 256, 16), F32),
        pltpu.VMEM((RES, 384, PAIR), F32),
        dma((NP,)), dma,
        dma((16, NP, 4)), dma((16, NP)), dma((4, NP, 2)), dma((4, NP)),
        dma((8, 4)), dma((2, 2, 8)), dma((4,)), dma((2, 2)),
    ]

    def local_fn(m, mask, z, gamma, beta, w_a, b_a, w_b, b_b, w_out, b_out):
        out = pl.pallas_call(
            kernel,
            out_shape=pltpu.VMEM((RES, 384, PAIR), F32),
            in_specs=[any_spec, vmem, any_spec] + [vmem] * 8,
            out_specs=vmem,
            scratch_shapes=scratch,
            compiler_params=pltpu.CompilerParams(
                collective_id=0, has_side_effects=True, vmem_limit_bytes=60 * 1024 * 1024),
            name="opm",
        )(jnp.transpose(m, (1, 0, 2)), mask.T, jnp.transpose(z, (1, 0, 2)), gamma, beta,
          w_a.T, b_a.reshape(1, HID), w_b.T, b_b.reshape(1, HID), w_out, b_out.reshape(1, PAIR))
        return jnp.transpose(out, (1, 0, 2))

    return jax.shard_map(local_fn, mesh=mesh, in_specs=in_specs, out_specs=row_spec, check_vma=False)
```

```python
import jax
import jax.numpy as jnp
from jax import lax
from jax.experimental import pallas as pl
from jax.experimental.pallas import tpu as pltpu
from jax.sharding import PartitionSpec as P

F32 = jnp.float32
BF16 = jnp.bfloat16
MESH = pl.DeviceIdType.MESH
NT = (((1,), (1,)), ((), ()))

SEQ, RES, CH, HID, PAIR = 512, 12, 256, 32, 128
PIECE = 128
NP = SEQ // PIECE
AROWS = RES * HID
PROWS = AROWS + 16
UNIT = 2 * RES

WAYS = ("x+", "x-", "y+", "y-", "z+", "z-")
MOVE = {"x+": (0, 0, 1), "x-": (0, 0, -1), "y+": (0, 1, 0), "y-": (0, -1, 0), "z+": (1, 0, 0), "z-": (-1, 0, 0)}
STEPS = ((0, 0), (0, 1), (1, 0), (3, 0), (1, 1), (3, 1), (2, 0), (2, 1))


def onward(place, p):
    dz, dy, dx = place
    plus = p < 2

    def along(d, axis):
        return [axis + "+"] if d == 1 and plus else [axis + "-"] if d == 3 and not plus else []

    if dz:
        return along(dz, "z")
    first, second, d1, d2 = ("x", "y", dx, dy) if p % 2 == 0 else ("y", "x", dy, dx)
    if d2:
        return along(d2, second)
    return along(d1, first) + [second + "+", second + "-"]


def all_hops():
    hops = [((0, 0, 0), p, way) for p in range(NP) for way in WAYS]
    for place, p, way in hops:
        to = tuple((a + b) % 4 for a, b in zip(place, MOVE[way]))
        for h in ((to, p, w) for w in onward(to, p)):
            if h not in hops:
                hops.append(h)
    return hops


ORDER = {-5: (0, 1, 2, 3, 4, 5), -4: (6, 8, 10), -3: (12, 13, 14, 15, 16, 17), -2: (18, 19, 7, 20, 9, 21, 22, 23, 11),
    -1: (24, 25, 26, 30, 27, 28, 31, 40, 34, 37, 33, 44, 41, 42, 45, 51, 35, 36, 38, 39, 46, 47, 32, 48, 49, 50, 61,
    62), 0: (52, 53), 1: (58, 54, 63), 2: (59, 29, 60, 64), 3: (56, 65, 67, 66, 57, 55, 43, 70), 4: (68,), 6: (69,
    71)}


def iota(shape, axis):
    return lax.broadcasted_iota(jnp.int32, shape, axis)


def dot(a, b, dims=None):
    if dims is None:
        return jnp.dot(a, b, preferred_element_type=F32)
    return lax.dot_general(a, b, dims, preferred_element_type=F32)


def kernel(m_hbm, mask_hbm, z_hbm, gamma_hbm, beta_hbm, wa_hbm, ba_hbm, wb_hbm, bb_hbm, wo_hbm, bo_hbm,
           out_ref,
           mask_ref, gamma_ref, beta_ref, wa_ref, ba_ref, wb_ref, bb_ref, wo_ref, bo_ref,
           m_v, mask_v, wabig, b32, a_buf, b_buf, bt, lhs2, rt, w32, wo_p, r_send, r_recv, n_send, n_recv,
           mask_all, inv_v, z_v,
           in_sem, m_sem, z_sem, a_ss, a_rs, b_ss, b_rs, r_ss, r_rs, n_ss, n_rs):
    col = lax.axis_index("col")
    dap = lax.axis_index("dap")
    zz, yy, xx = col // 16, (col // 4) % 4, col % 4
    home = zz // 2
    other = 1 - dap

    def at(dz=0, dy=0, dx=0):
        return ((zz + dz) % 4) * 16 + ((yy + dy) % 4) * 4 + (xx + dx) % 4

    def dev(c, d):
        return {"col": c, "dap": d}

    small = [pltpu.make_async_copy(src, dst, in_sem.at[i]) for i, (src, dst) in enumerate((
        (mask_hbm, mask_ref), (gamma_hbm, gamma_ref), (beta_hbm, beta_ref), (wa_hbm, wa_ref), (ba_hbm, ba_ref),
        (wb_hbm, wb_ref), (bb_hbm, bb_ref), (wo_hbm, wo_ref), (bo_hbm, bo_ref)))]
    for p in range(NP):
        pltpu.make_async_copy(m_hbm.at[:, pl.ds(PIECE * p, PIECE), :], m_v.at[p], m_sem.at[p]).start()
        if p == 0:
            for copy in small:
                copy.start()
    barrier = pltpu.get_barrier_semaphore()
    greet = [dev(at(dy=1), dap), dev(at(dy=3), dap), dev(at(dx=1), dap), dev(at(dx=3), dap), dev(col, other)]
    for r in (1, 2, 3):
        for d in (0, 1):
            greet.append(dev(at(dz=r), d))
    for who in greet:
        pl.semaphore_signal(barrier, inc=1, device_id=who, device_id_type=MESH)

    for copy in small:
        copy.wait()
    mask_v[...] = jnp.zeros_like(mask_v)
    mask_v[0:RES, :] = mask_ref[...].astype(F32)
    wa = wa_ref[...]
    for k in range(4):
        rows = [wa if kk == k else jnp.zeros_like(wa) for kk in range(4)]
        wabig[:, CH * k:CH * (k + 1)] = jnp.concatenate(rows, axis=0)
    gamma = gamma_ref[...].astype(F32).reshape(1, CH)
    beta = beta_ref[...].astype(F32).reshape(1, CH)
    tile4 = jnp.where(iota((HID, 128), 1) % HID == iota((HID, 128), 0), 1.0, 0.0).astype(BF16)
    ba_row = dot(jnp.broadcast_to(ba_ref[...], (16, HID)), tile4)[0:1, :]
    eye = iota((HID, HID), 0) == iota((HID, HID), 1)
    bb_diag = jnp.where(eye, jnp.broadcast_to(bb_ref[...], (HID, HID)).astype(F32), 0.0).astype(BF16)
    bb_col = dot(bb_diag, jnp.ones((HID, 128), BF16))

    def hop(place, p, way):
        to = tuple((d + s) % 4 for d, s in zip(place, MOVE[way]))
        w = WAYS.index(way) % 4 % 2 + 2 * (way[0] == "y")
        if way[0] == "z":
            return pltpu.make_async_remote_copy(
                src_ref=b_buf.at[place[0], p], dst_ref=b_buf.at[to[0], p], send_sem=b_ss.at[place[0], p, w],
                recv_sem=b_rs.at[to[0], p], device_id=dev(at(*MOVE[way]), dap), device_id_type=MESH)
        src, dst = place[1] * 4 + place[2], to[1] * 4 + to[2]
        return pltpu.make_async_remote_copy(
            src_ref=a_buf.at[src, p], dst_ref=a_buf.at[dst, p], send_sem=a_ss.at[src, p, w],
            recv_sem=a_rs.at[dst, p], device_id=dev(at(*MOVE[way]), dap), device_id_type=MESH)

    def wait_a(i, p):
        pltpu.make_async_remote_copy(
            src_ref=a_buf.at[i, p], dst_ref=a_buf.at[i, p], send_sem=a_ss.at[i, p, 0], recv_sem=a_rs.at[i, p],
            device_id=dev(at(dx=1), dap), device_id_type=MESH).wait_recv()

    def wait_b(r, p):
        pltpu.make_async_remote_copy(
            src_ref=b_buf.at[r, p], dst_ref=b_buf.at[r, p], send_sem=b_ss.at[r, p, 0], recv_sem=b_rs.at[r, p],
            device_id=dev(at(dz=1), dap), device_id_type=MESH).wait_recv()

    hops = all_hops()
    sent, seen = [], set()

    def need(place, p):
        if any(place) and (place, p) not in seen:
            seen.add((place, p))
            if place[0]:
                wait_b(place[0], p)
            else:
                wait_a(place[1] * 4 + place[2], p)

    def run(key):
        for i in ORDER.get(key, ()):
            place, p, way = hops[i]
            need(place, p)
            hop(place, p, way).start()
            sent.append((place, p, way))

    def project(p, carry):
        pltpu.make_async_copy(m_hbm.at[:, pl.ds(0, PIECE), :], m_v.at[p], m_sem.at[p]).wait()
        lanes = pl.ds(pl.multiple_of(PIECE * p, PIECE), PIECE)
        mask_p = mask_v[:, lanes]
        mask_b = mask_p.astype(BF16)
        mask_t = mask_p.T.astype(BF16)
        for q in range(3):
            xs = []
            for k in range(4):
                n = 4 * q + k
                v = m_v[p, n].astype(F32)
                mean = jnp.sum(v, axis=1, keepdims=True) * (1.0 / CH)
                cen = v - mean
                var = jnp.sum(cen * cen, axis=1, keepdims=True) * (1.0 / CH)
                x = (cen * lax.rsqrt(var + 1e-5) * gamma + beta).astype(BF16)
                xs.append(x)
                lin_b = dot(wb_ref[...], x, NT)
                b32[pl.ds(n, HID, stride=RES), :] = (lin_b + bb_col) * mask_p[n:n + 1, :]
            lin_a = dot(jnp.concatenate(xs, axis=1), wabig[...], NT)
            spread = jnp.where(iota((16, 128), 1) // HID + 4 * q == iota((16, 128), 0), 1.0, 0.0).astype(BF16)
            a_buf[0, p, 128 * q:128 * (q + 1), :] = ((lin_a + ba_row) * dot(mask_t, spread)).astype(BF16)
        a_buf[0, p, AROWS:PROWS, :] = mask_b
        b_buf[0, p, 0:AROWS, :] = b32[...].astype(BF16)
        b_buf[0, p, AROWS:PROWS, :] = mask_b

        @pl.when(p == 0)
        def _():
            pl.semaphore_wait(barrier, len(greet))

        for k in range(NP):
            @pl.when(p == k)
            def _(k=k):
                run(k - 5)
        return carry

    lax.fori_loop(0, NP, project, 0)
    pltpu.make_async_copy(z_hbm, z_v, z_sem).start()

    w32[...] = wo_ref[...].astype(F32)

    def order(d, carry):
        wo_p[pl.ds(pl.multiple_of(HID * d, HID), HID), :] = w32[pl.ds(d, HID, stride=HID), :].astype(BF16)
        return carry

    lax.fori_loop(0, HID, order, 0)

    run(-1)

    for r in (1, 3, 2):
        for p in range(NP):
            need((r, 0, 0), p)
    n192 = 4 * 4 * RES
    ro, co = iota((n192, n192), 0), iota((n192, n192), 1)
    want = ((ro // RES) % 4) * 48 + (ro // 48) * RES + ro % RES
    perm = jnp.where(want == co, 1.0, 0.0).astype(BF16)

    for g in range(8):
        cat = jnp.concatenate(
            [jnp.concatenate([b_buf[r, p, 48 * g:48 * (g + 1), :] for p in range(NP)], axis=1) for r in range(4)], axis=0)
        bt[n192 * g:n192 * (g + 1), :] = dot(perm, cat).astype(BF16)

    lane = iota((1, 128), 1)
    low = lane < 64
    odd = (lane // HID) % 2 == 1

    def transpose4(v):
        def swap(u, w):
            t = pltpu.roll(jnp.where(low, w, u), 64, 1)
            return jnp.where(low, u, t), jnp.where(low, t, w)

        def swap2(u, w):
            return (jnp.where(odd, pltpu.roll(w, 32, 1), u), jnp.where(odd, w, pltpu.roll(u, 96, 1)))

        e0, e2 = swap(v[0], v[2])
        e1, e3 = swap(v[1], v[3])
        w0, w1 = swap2(e0, e1)
        w2, w3 = swap2(e2, e3)
        return w0, w1, w2, w3

    def r_copy(t, r, unit):
        return pltpu.make_async_remote_copy(
            src_ref=r_send.at[t, r], dst_ref=r_recv.at[zz % 2, dap, unit], send_sem=r_ss.at[t, r],
            recv_sem=r_rs.at[zz % 2, dap, unit], device_id=dev(at(dz=-r), home), device_id_type=MESH)

    def n_copy(r):
        return pltpu.make_async_remote_copy(
            src_ref=n_send.at[r], dst_ref=n_recv.at[zz % 2, dap], send_sem=n_ss.at[r],
            recv_sem=n_rs.at[zz % 2, dap], device_id=dev(at(dz=-r), home), device_id_type=MESH)

    def count():
        for dy in range(4):
            for dx in range(4):
                pos = ((yy + 4 - dy) % 4) * 4 + (xx + 4 - dx) % 4
                mask_all[pl.ds(pl.multiple_of(16 * pos, 16), 16), :] = jnp.concatenate(
                    [a_buf[dy * 4 + dx, p, AROWS:PROWS, :] for p in range(NP)], axis=1)
        ro, co = iota((256, 256), 0), iota((256, 256), 1)
        squeeze = jnp.where((ro < 192) & ((ro // RES) * 16 + ro % RES == co), 1.0, 0.0).astype(BF16)
        mask_rows = dot(squeeze, mask_all[...]).astype(BF16)
        for r in range(4):
            mask_cols = jnp.concatenate([b_buf[r, p, AROWS:PROWS, :] for p in range(NP)], axis=1)
            part = dot(mask_cols, mask_rows, NT)
            if r:
                n_send[r] = part
                n_copy(r).start()
            else:
                @pl.when(home == dap)
                def _(part=part):
                    n_recv[zz % 2, dap] = part

                @pl.when(home != dap)
                def _(part=part):
                    n_send[0] = part
                    n_copy(0).start()

    rest = {0: (), 1: (2,), 3: (0,), 2: (0, 2)}
    px = 3 - 2 * (xx % 2)

    def place(t):
        dy, far = jnp.int32(STEPS[7][0]), jnp.int32(STEPS[7][1])
        for i in range(6, -1, -1):
            dy = jnp.where(t == i, STEPS[i][0], dy)
            far = jnp.where(t == i, STEPS[i][1], far)
        pair = (xx // 2 + far) % 2
        return dy, pair, ((yy + 4 - dy) % 4) * 2 + pair

    def step(t, carry):
        for at_t in range(8):
            @pl.when(t == at_t)
            def _(at_t=at_t):
                run(at_t)
                dy, far = STEPS[at_t]
                for dx in (2 * far, 1, 3):
                    for p in range(NP):
                        if onward((0, dy, dx), p):
                            need((0, dy, dx), p)
                if not far:
                    for p in rest[dy]:
                        wait_a(dy * 4, p)
                    near, p = dy * 4 + px, 4 - px
                else:
                    for p in rest[dy] + (1, 3):
                        wait_a(dy * 4 + 2, p)
                    near, p = dy * 4 + 4 - px, px
                for q in rest[dy]:
                    wait_a(near, q)
                wait_a(near, p)
                if at_t == 7:
                    count()

        dy, pair, unit = place(t)
        slots = [dy * 4 + (xx + 4 - (2 * pair + o)) % 4 for o in range(2)]

        for c in range(3):
            quads = (2 * c, 2 * c + 1)
            rhs = jnp.concatenate(
                [jnp.concatenate([a_buf[slots[q // 3], p, 128 * (q % 3):128 * (q % 3 + 1), :] for q in quads], axis=1)
                 for p in range(NP)], axis=0)
            for g in range(2):
                prod = dot(bt[4 * n192 * g:4 * n192 * (g + 1), :], rhs)
                for h in range(4):
                    for k2, q in enumerate(quads):
                        base = n192 * h
                        v = [prod[base + 48 * d:base + 48 * (d + 1), 128 * k2:128 * (k2 + 1)] for d in range(4)]
                        for k, w in enumerate(transpose4(v)):
                            i = 4 * q + k
                            lhs2[4 * g + h, 48 * i:48 * (i + 1), :] = w.astype(BF16)
        res = dot(jnp.concatenate([lhs2[g] for g in range(8)], axis=1), wo_p[...])
        for i in range(UNIT):
            for jg in range(6):
                rt[pl.ds(8 * jg * UNIT + i, 8, stride=UNIT), :] = res[48 * i + 8 * jg:48 * i + 8 * jg + 8, :]
        own = rt[0:RES * UNIT, :].astype(BF16)

        @pl.when(home == dap)
        def _():
            r_recv[zz % 2, dap, unit] = own

        for r in (2, 1, 3):
            r_send[t, r] = rt[RES * UNIT * r:RES * UNIT * (r + 1), :].astype(BF16)
            r_copy(t, r, unit).start()

        @pl.when(home != dap)
        def _():
            r_send[t, 0] = own
            r_copy(t, 0, unit).start()
        return carry

    lax.fori_loop(0, 8, step, 0)

    pltpu.make_async_copy(z_hbm, z_v, z_sem).wait()
    bo = bo_ref[...].astype(F32)

    def arrive(ref, sem, src):
        pltpu.make_async_remote_copy(
            src_ref=src, dst_ref=ref, send_sem=n_ss.at[0], recv_sem=sem,
            device_id=dev(col, other), device_id_type=MESH).wait_recv()

    for k in range(2):
        for c in range(2):
            @pl.when(jnp.logical_not((zz == 2 * dap + k) & (dap == c)))
            def _(k=k, c=c):
                arrive(n_recv.at[k, c], n_rs.at[k, c], n_send.at[0])
        inv = 1.0 / (1e-3 + (n_recv[k, 0] + n_recv[k, 1]))
        inv_v[k] = inv.T

    def finish(t, carry):
        _, _, u = place(t)
        for k in range(2):
            for c in range(2):
                @pl.when(jnp.logical_not((zz == 2 * dap + k) & (dap == c)))
                def _(k=k, c=c):
                    arrive(r_recv.at[k, c, u], r_rs.at[k, c, u], r_send.at[0, 0])
            rows = pl.ds(pl.multiple_of(UNIT * u, 8), UNIT)
            dst = pl.ds(pl.multiple_of(192 * k + UNIT * u, 8), UNIT)
            inv = inv_v[k, rows, :]
            total = r_recv[k, 0, u].astype(F32) + r_recv[k, 1, u].astype(F32) + bo
            for j in range(RES):
                out_ref[j, dst, :] = z_v[j, dst, :] + total[UNIT * j:UNIT * (j + 1), :] * inv[:, j:j + 1]
        return carry

    lax.fori_loop(0, 8, finish, 0)

    for place, p, way in sent:
        hop(place, p, way).wait_send()

    def left(t, carry):
        for r in (1, 2, 3):
            r_copy(t, r, 0).wait_send()

        @pl.when(home != dap)
        def _():
            r_copy(t, 0, 0).wait_send()
        return carry

    lax.fori_loop(0, 8, left, 0)
    for r in (1, 2, 3):
        n_copy(r).wait_send()

    @pl.when(home != dap)
    def _():
        n_copy(0).wait_send()


def solution(mesh):
    row_spec = P(("data", "dap"), "col", None)
    mask_spec = P(("data", "dap"), "col")
    in_specs = (row_spec, mask_spec, row_spec) + (P(),) * 8
    any_spec = pl.BlockSpec(memory_space=pl.ANY)
    vmem = pl.BlockSpec(memory_space=pltpu.VMEM)
    dma = pltpu.SemaphoreType.DMA
    scratch = [
        pltpu.VMEM((RES, SEQ), jnp.int32), pltpu.VMEM((CH,), BF16), pltpu.VMEM((CH,), BF16), pltpu.VMEM((HID, CH), BF16),
        pltpu.VMEM((1, HID), BF16), pltpu.VMEM((HID, CH), BF16), pltpu.VMEM((1, HID), BF16),
        pltpu.VMEM((HID * HID, PAIR), BF16), pltpu.VMEM((1, PAIR), BF16),
        pltpu.VMEM((NP, RES, PIECE, CH), BF16),
        pltpu.VMEM((16, SEQ), F32),
        pltpu.VMEM((128, 4 * CH), BF16),
        pltpu.VMEM((AROWS, PIECE), F32),
        pltpu.VMEM((16, NP, PROWS, 128), BF16),
        pltpu.VMEM((4, NP, PROWS, 128), BF16),
        pltpu.VMEM((4 * AROWS, SEQ), BF16),
        pltpu.VMEM((8, UNIT * 48, 128), BF16),
        pltpu.VMEM((48 * UNIT, PAIR), F32),
        pltpu.VMEM((HID * HID, PAIR), F32),
        pltpu.VMEM((HID * HID, PAIR), BF16),
        pltpu.VMEM((8, 4, RES * UNIT, PAIR), BF16),
        pltpu.VMEM((2, 2, 8, RES * UNIT, PAIR), BF16),
        pltpu.VMEM((4, 16, 256), F32),
        pltpu.VMEM((2, 2, 16, 256), F32),
        pltpu.VMEM((256, SEQ), BF16),
        pltpu.VMEM((2, 256, 16), F32),
        pltpu.VMEM((RES, 384, PAIR), F32),
        dma((9,)), dma((NP,)), dma,
        dma((16, NP, 4)), dma((16, NP)), dma((4, NP, 2)), dma((4, NP)),
        dma((8, 4)), dma((2, 2, 8)), dma((4,)), dma((2, 2)),
    ]

    def local_fn(m, mask, z, gamma, beta, w_a, b_a, w_b, b_b, w_out, b_out):
        out = pl.pallas_call(
            kernel,
            out_shape=pltpu.VMEM((RES, 384, PAIR), F32),
            in_specs=[any_spec] * 11,
            out_specs=vmem,
            scratch_shapes=scratch,
            compiler_params=pltpu.CompilerParams(
                collective_id=0, has_side_effects=True, vmem_limit_bytes=60 * 1024 * 1024),
            name="opm",
        )(jnp.transpose(m, (1, 0, 2)), mask.T, jnp.transpose(z, (1, 0, 2)), gamma, beta,
          w_a.T, b_a.reshape(1, HID), w_b.T, b_b.reshape(1, HID), w_out, b_out.reshape(1, PAIR))
        return jnp.transpose(out, (1, 0, 2))

    return jax.shard_map(local_fn, mesh=mesh, in_specs=in_specs, out_specs=row_spec, check_vma=False)
```

```python
import jax
import jax.numpy as jnp
from jax import lax
from jax.experimental import pallas as pl
from jax.experimental.pallas import tpu as pltpu
from jax.sharding import PartitionSpec as P

F32 = jnp.float32
BF16 = jnp.bfloat16
MESH = pl.DeviceIdType.MESH
NT = (((1,), (1,)), ((), ()))

SEQ, RES, CH, HID, PAIR = 512, 12, 256, 32, 128
LANES = 128
PIECE = 128
NP = SEQ // PIECE
AROWS = RES * HID
PROWS = AROWS + 16
UNIT = 2 * RES

WAYS = ("x+", "x-", "y+", "y-", "z+", "z-")
MOVE = {w: tuple((w[0] == ax) * (1 if w[1] == "+" else -1) for ax in "zyx") for w in WAYS}
STEPS = ((0, 0), (0, 1), (1, 0), (3, 0), (1, 1), (3, 1), (2, 0), (2, 1))


PLUS = {"x": (1, 2), "y": (2, 3), "z": (0, 1)}


def onward(place, p):
    dz, dy, dx = place

    def along(d, axis):
        if d == 1 and p in PLUS[axis]:
            return [axis + "+"]
        return [axis + "-"] if d == 3 and p not in PLUS[axis] else []

    if dz:
        return along(dz, "z")
    first, second, d1, d2 = ("y", "x", dy, dx) if p % 2 else ("x", "y", dx, dy)
    if d2:
        return along(d2, second)
    return along(d1, first) + [second + "+", second + "-"]


def all_hops():
    hops = [((0, 0, 0), p, way) for p in range(NP) for way in WAYS]
    for place, p, way in hops:
        to = tuple((a + b) % 4 for a, b in zip(place, MOVE[way]))
        for h in ((to, p, w) for w in onward(to, p)):
            if h not in hops:
                hops.append(h)
    return hops


ORDER = {-5: (0, 1, 2, 3, 4, 5), -4: (6, 7, 8, 9, 10), -3: (17,), -2: (12, 19, 14, 15, 22, 23), -1: (18, 13, 20, 21,
    16, 11, 26, 24, 28, 30, 31, 44, 32, 33, 27, 25, 37, 51, 38, 45, 39, 40, 47, 48, 41, 42, 49, 50, 46, 34), 1: (35,
    36, 60, 61), 2: (56, 66, 53, 55, 43, 54), 3: (57, 65, 62, 29, 59, 67), 4: (64, 58, 63, 52), 5: (69, 71, 70, 68)}


def iota(shape, axis):
    return lax.broadcasted_iota(jnp.int32, shape, axis)


def dot(a, b, dims=None):
    if dims is None:
        return jnp.dot(a, b, preferred_element_type=F32)
    return lax.dot_general(a, b, dims, preferred_element_type=F32)


def kernel(m_hbm, mask_hbm, z_hbm, gamma_hbm, beta_hbm, wa_hbm, ba_hbm, wb_hbm, bb_hbm, wo_hbm, bo_hbm,
           out_ref,
           mask_ref, gamma_ref, beta_ref, wa_ref, ba_ref, wb_ref, bb_ref, wo_ref, bo_ref,
           m_v, mask_v, wabig, b32, a_buf, b_buf, bt, lhs2, rt, w32, wo_p, r_send, r_recv, n_send, n_recv,
           mask_all, inv_v, z_v,
           in_sem, m_sem, z_sem, a_ss, a_rs, b_ss, b_rs, r_ss, r_rs, n_ss, n_rs):
    col = lax.axis_index("col")
    dap = lax.axis_index("dap")
    zz, yy, xx = col // 16, (col // 4) % 4, col % 4
    home = zz // 2
    other = 1 - dap

    def at(dz=0, dy=0, dx=0):
        return ((zz + dz) % 4) * 16 + ((yy + dy) % 4) * 4 + (xx + dx) % 4

    def dev(c, d):
        return {"col": c, "dap": d}

    small = [pltpu.make_async_copy(src, dst, in_sem.at[i]) for i, (src, dst) in enumerate((
        (mask_hbm, mask_ref), (gamma_hbm, gamma_ref), (beta_hbm, beta_ref), (wa_hbm, wa_ref), (ba_hbm, ba_ref),
        (wb_hbm, wb_ref), (bb_hbm, bb_ref), (wo_hbm, wo_ref), (bo_hbm, bo_ref)))]
    for p in range(NP):
        pltpu.make_async_copy(m_hbm.at[:, pl.ds(PIECE * p, PIECE), :], m_v.at[p], m_sem.at[p]).start()
        if p == 0:
            for copy in small:
                copy.start()
    barrier = pltpu.get_barrier_semaphore()
    greet = [dev(at(dy=1), dap), dev(at(dy=3), dap), dev(at(dx=1), dap), dev(at(dx=3), dap), dev(col, other)]
    for r in (1, 2, 3):
        for d in (0, 1):
            greet.append(dev(at(dz=r), d))
    for who in greet:
        pl.semaphore_signal(barrier, inc=1, device_id=who, device_id_type=MESH)

    for copy in small:
        copy.wait()
    mask_v[...] = jnp.zeros_like(mask_v)
    mask_v[0:RES, :] = mask_ref[...].astype(F32)
    wa = wa_ref[...]
    for k in range(4):
        rows = [wa if kk == k else jnp.zeros_like(wa) for kk in range(4)]
        wabig[:, CH * k:CH * (k + 1)] = jnp.concatenate(rows, axis=0)
    gamma = gamma_ref[...].astype(F32).reshape(1, CH)
    beta = beta_ref[...].astype(F32).reshape(1, CH)
    tile4 = jnp.where(iota((HID, LANES), 1) % HID == iota((HID, LANES), 0), 1.0, 0.0).astype(BF16)
    ba_row = dot(jnp.broadcast_to(ba_ref[...], (16, HID)), tile4)[0:1, :]
    eye = iota((HID, HID), 0) == iota((HID, HID), 1)
    bb_diag = jnp.where(eye, jnp.broadcast_to(bb_ref[...], (HID, HID)).astype(F32), 0.0).astype(BF16)
    bb_col = dot(bb_diag, jnp.ones((HID, LANES), BF16))

    def hop(place, p, way):
        to = tuple((d + s) % 4 for d, s in zip(place, MOVE[way]))
        if way[0] == "z":
            return pltpu.make_async_remote_copy(
                src_ref=b_buf.at[place[0], p], dst_ref=b_buf.at[to[0], p], send_sem=b_ss,
                recv_sem=b_rs.at[to[0], p], device_id=dev(at(*MOVE[way]), dap), device_id_type=MESH)
        src, dst = place[1] * 4 + place[2], to[1] * 4 + to[2]
        return pltpu.make_async_remote_copy(
            src_ref=a_buf.at[src, p], dst_ref=a_buf.at[dst, p], send_sem=a_ss,
            recv_sem=a_rs.at[dst, p], device_id=dev(at(*MOVE[way]), dap), device_id_type=MESH)

    def wait_a(i, p):
        pltpu.make_async_remote_copy(
            src_ref=a_buf.at[i, p], dst_ref=a_buf.at[i, p], send_sem=a_ss, recv_sem=a_rs.at[i, p],
            device_id=dev(at(dx=1), dap), device_id_type=MESH).wait_recv()

    def wait_b(r, p):
        pltpu.make_async_remote_copy(
            src_ref=b_buf.at[r, p], dst_ref=b_buf.at[r, p], send_sem=b_ss, recv_sem=b_rs.at[r, p],
            device_id=dev(at(dz=1), dap), device_id_type=MESH).wait_recv()

    hops = all_hops()
    seen = set()

    def need(place, p):
        if any(place) and (place, p) not in seen:
            seen.add((place, p))
            if place[0]:
                wait_b(place[0], p)
            else:
                wait_a(place[1] * 4 + place[2], p)

    def run(key):
        for i in ORDER.get(key, ()):
            place, p, way = hops[i]
            need(place, p)
            hop(place, p, way).start()

    def project(p, carry):
        pltpu.make_async_copy(m_hbm.at[:, pl.ds(0, PIECE), :], m_v.at[p], m_sem.at[p]).wait()
        lanes = pl.ds(pl.multiple_of(PIECE * p, PIECE), PIECE)
        mask_p = mask_v[:, lanes]
        mask_b = mask_p.astype(BF16)
        mask_t = mask_p.T.astype(BF16)
        for q in range(3):
            xs = []
            for k in range(4):
                n = 4 * q + k
                v = m_v[p, n].astype(F32)
                mean = jnp.sum(v, axis=1, keepdims=True) * (1.0 / CH)
                cen = v - mean
                var = jnp.sum(cen * cen, axis=1, keepdims=True) * (1.0 / CH)
                x = (cen * lax.rsqrt(var + 1e-5) * gamma + beta).astype(BF16)
                xs.append(x)
                lin_b = dot(wb_ref[...], x, NT)
                b32[pl.ds(n, HID, stride=RES), :] = (lin_b + bb_col) * mask_p[n:n + 1, :]
            lin_a = dot(jnp.concatenate(xs, axis=1), wabig[...], NT)
            spread = jnp.where(iota((16, LANES), 1) // HID + 4 * q == iota((16, LANES), 0), 1.0, 0.0).astype(BF16)
            a_buf[0, p, LANES * q:LANES * (q + 1), :] = ((lin_a + ba_row) * dot(mask_t, spread)).astype(BF16)
        a_buf[0, p, AROWS:PROWS, :] = mask_b
        b_buf[0, p, 0:AROWS, :] = b32[...].astype(BF16)
        b_buf[0, p, AROWS:PROWS, :] = mask_b

        @pl.when(p == 0)
        def _():
            pl.semaphore_wait(barrier, len(greet))

        for k in range(NP):
            @pl.when(p == k)
            def _(k=k):
                run(k - 5)
        return carry

    lax.fori_loop(0, NP, project, 0)
    pltpu.make_async_copy(z_hbm, z_v, z_sem).start()

    w32[...] = wo_ref[...].astype(F32)

    def order(d, carry):
        wo_p[pl.ds(pl.multiple_of(HID * d, HID), HID), :] = w32[pl.ds(d, HID, stride=HID), :].astype(BF16)
        return carry

    lax.fori_loop(0, HID, order, 0)

    run(-1)

    for r in (1, 3, 2):
        for p in range(NP):
            need((r, 0, 0), p)
    n192 = 4 * 4 * RES
    ro, co = iota((n192, n192), 0), iota((n192, n192), 1)
    want = ((ro // RES) % 4) * 48 + (ro // 48) * RES + ro % RES
    perm = jnp.where(want == co, 1.0, 0.0).astype(BF16)

    for g in range(8):
        cat = jnp.concatenate(
            [jnp.concatenate([b_buf[r, p, 48 * g:48 * (g + 1), :] for p in range(NP)], axis=1) for r in range(4)], axis=0)
        bt[n192 * g:n192 * (g + 1), :] = dot(perm, cat).astype(BF16)

    lane = iota((1, LANES), 1)
    low = lane < 64
    odd = (lane // HID) % 2 == 1

    def transpose4(v):
        def swap(u, w):
            t = pltpu.roll(jnp.where(low, w, u), 64, 1)
            return jnp.where(low, u, t), jnp.where(low, t, w)

        def swap2(u, w):
            return (jnp.where(odd, pltpu.roll(w, 32, 1), u), jnp.where(odd, w, pltpu.roll(u, 96, 1)))

        e0, e2 = swap(v[0], v[2])
        e1, e3 = swap(v[1], v[3])
        w0, w1 = swap2(e0, e1)
        w2, w3 = swap2(e2, e3)
        return w0, w1, w2, w3

    def r_copy(t, r, unit):
        return pltpu.make_async_remote_copy(
            src_ref=r_send.at[t, r], dst_ref=r_recv.at[zz % 2, dap, unit], send_sem=r_ss.at[1 if r else 0],
            recv_sem=r_rs.at[zz % 2, dap, unit], device_id=dev(at(dz=-r), home), device_id_type=MESH)

    def n_copy(r):
        return pltpu.make_async_remote_copy(
            src_ref=n_send.at[r], dst_ref=n_recv.at[zz % 2, dap], send_sem=n_ss.at[1 if r else 0],
            recv_sem=n_rs.at[zz % 2, dap], device_id=dev(at(dz=-r), home), device_id_type=MESH)

    def count():
        for dy in range(4):
            for dx in range(4):
                pos = ((yy + 4 - dy) % 4) * 4 + (xx + 4 - dx) % 4
                mask_all[pl.ds(pl.multiple_of(16 * pos, 16), 16), :] = jnp.concatenate(
                    [a_buf[dy * 4 + dx, p, AROWS:PROWS, :] for p in range(NP)], axis=1)
        ro, co = iota((256, 256), 0), iota((256, 256), 1)
        squeeze = jnp.where((ro < 192) & ((ro // RES) * 16 + ro % RES == co), 1.0, 0.0).astype(BF16)
        mask_rows = dot(squeeze, mask_all[...]).astype(BF16)
        for r in range(4):
            mask_cols = jnp.concatenate([b_buf[r, p, AROWS:PROWS, :] for p in range(NP)], axis=1)
            part = dot(mask_cols, mask_rows, NT)
            if r:
                n_send[r] = part
                n_copy(r).start()
            else:
                @pl.when(home == dap)
                def _(part=part):
                    n_recv[zz % 2, dap] = part

                @pl.when(home != dap)
                def _(part=part):
                    n_send[0] = part
                    n_copy(0).start()

    stay = [p for d in (1, 3) for p in (1, 3) if not onward((0, 1, d), p)]
    px = 3 - 2 * (xx % 2)

    def place(t):
        dy, far = jnp.int32(STEPS[7][0]), jnp.int32(STEPS[7][1])
        for i in range(6, -1, -1):
            dy = jnp.where(t == i, STEPS[i][0], dy)
            far = jnp.where(t == i, STEPS[i][1], far)
        pair = (xx // 2 + far) % 2
        return dy, pair, ((yy + 4 - dy) % 4) * 2 + pair

    def step(t, carry):
        for at_t in range(8):
            @pl.when(t == at_t)
            def _(at_t=at_t):
                run(at_t)
                dy, far = STEPS[at_t]
                rest = [p for p in (0, 2) if dy and not onward((0, dy, 1), p)]
                for dx in (2 * far, 1, 3):
                    for p in range(NP):
                        if onward((0, dy, dx), p):
                            need((0, dy, dx), p)
                near = 4 - px if far else px
                for p in rest + [1, 3] * far:
                    if dy or far:
                        wait_a(dy * 4 + 2 * far, p)
                for q in rest:
                    wait_a(dy * 4 + near, q)
                wait_a(dy * 4 + near, jnp.where(near == 1, stay[0], stay[1]))
                if at_t == 7:
                    count()

        dy, pair, unit = place(t)
        slots = [dy * 4 + (xx + 4 - (2 * pair + o)) % 4 for o in range(2)]

        for c in range(3):
            quads = (2 * c, 2 * c + 1)
            rhs = jnp.concatenate(
                [jnp.concatenate([a_buf[slots[q // 3], p, LANES * (q % 3):LANES * (q % 3 + 1), :] for q in quads], axis=1)
                 for p in range(NP)], axis=0)
            for g in range(2):
                prod = dot(bt[4 * n192 * g:4 * n192 * (g + 1), :], rhs)
                for h in range(4):
                    for k2, q in enumerate(quads):
                        base = n192 * h
                        v = [prod[base + 48 * d:base + 48 * (d + 1), LANES * k2:LANES * (k2 + 1)] for d in range(4)]
                        for k, w in enumerate(transpose4(v)):
                            i = 4 * q + k
                            lhs2[4 * g + h, 48 * i:48 * (i + 1), :] = w.astype(BF16)
        res = dot(jnp.concatenate([lhs2[g] for g in range(8)], axis=1), wo_p[...])
        for i in range(UNIT):
            for jg in range(6):
                rt[pl.ds(8 * jg * UNIT + i, 8, stride=UNIT), :] = res[48 * i + 8 * jg:48 * i + 8 * jg + 8, :]
        own = rt[0:RES * UNIT, :].astype(BF16)

        @pl.when(home == dap)
        def _():
            r_recv[zz % 2, dap, unit] = own

        for r in (2, 1, 3):
            r_send[t, r] = rt[RES * UNIT * r:RES * UNIT * (r + 1), :].astype(BF16)
            r_copy(t, r, unit).start()

        @pl.when(home != dap)
        def _():
            r_send[t, 0] = own
            r_copy(t, 0, unit).start()
        return carry

    lax.fori_loop(0, 8, step, 0)

    pltpu.make_async_copy(z_hbm, z_v, z_sem).wait()
    bo = bo_ref[...].astype(F32)

    def arrive(ref, sem, src):
        pltpu.make_async_remote_copy(
            src_ref=src, dst_ref=ref, send_sem=n_ss.at[0], recv_sem=sem,
            device_id=dev(col, other), device_id_type=MESH).wait_recv()

    for k in range(2):
        for c in range(2):
            @pl.when(jnp.logical_not((zz == 2 * dap + k) & (dap == c)))
            def _(k=k, c=c):
                arrive(n_recv.at[k, c], n_rs.at[k, c], n_send.at[0])
        inv = 1.0 / (1e-3 + (n_recv[k, 0] + n_recv[k, 1]))
        inv_v[k] = inv.T

    def finish(t, carry):
        _, _, u = place(t)
        for k in range(2):
            for c in range(2):
                @pl.when(jnp.logical_not((zz == 2 * dap + k) & (dap == c)))
                def _(k=k, c=c):
                    arrive(r_recv.at[k, c, u], r_rs.at[k, c, u], r_send.at[0, 0])
            rows = pl.ds(pl.multiple_of(UNIT * u, 8), UNIT)
            dst = pl.ds(pl.multiple_of(192 * k + UNIT * u, 8), UNIT)
            inv = inv_v[k, rows, :]
            total = r_recv[k, 0, u].astype(F32) + r_recv[k, 1, u].astype(F32) + bo
            for j in range(RES):
                out_ref[j, dst, :] = z_v[j, dst, :] + total[UNIT * j:UNIT * (j + 1), :] * inv[:, j:j + 1]
        return carry

    lax.fori_loop(0, 8, finish, 0)

    def left(ref, sem):
        pltpu.make_async_remote_copy(src_ref=ref, dst_ref=ref, send_sem=sem, recv_sem=n_rs.at[0, 0],
                                     device_id=dev(col, other), device_id_type=MESH).wait_send()

    left(a_buf.at[pl.ds(0, 15)], a_ss)
    left(b_buf.at[pl.ds(0, 3)], b_ss)
    left(r_send.at[pl.ds(0, 6)], r_ss.at[1])
    left(n_send.at[pl.ds(0, 3)], n_ss.at[1])

    @pl.when(home != dap)
    def _():
        left(r_send.at[pl.ds(0, 2)], r_ss.at[0])
        left(n_send.at[pl.ds(0, 1)], n_ss.at[0])


def solution(mesh):
    row_spec = P(("data", "dap"), "col", None)
    mask_spec = P(("data", "dap"), "col")
    in_specs = (row_spec, mask_spec, row_spec) + (P(),) * 8
    any_spec = pl.BlockSpec(memory_space=pl.ANY)
    vmem = pl.BlockSpec(memory_space=pltpu.VMEM)
    dma = pltpu.SemaphoreType.DMA
    scratch = [
        pltpu.VMEM((RES, SEQ), jnp.int32), pltpu.VMEM((CH,), BF16), pltpu.VMEM((CH,), BF16), pltpu.VMEM((HID, CH), BF16),
        pltpu.VMEM((1, HID), BF16), pltpu.VMEM((HID, CH), BF16), pltpu.VMEM((1, HID), BF16),
        pltpu.VMEM((HID * HID, PAIR), BF16), pltpu.VMEM((1, PAIR), BF16),
        pltpu.VMEM((NP, RES, PIECE, CH), BF16),
        pltpu.VMEM((16, SEQ), F32),
        pltpu.VMEM((LANES, 4 * CH), BF16),
        pltpu.VMEM((AROWS, PIECE), F32),
        pltpu.VMEM((16, NP, PROWS, LANES), BF16),
        pltpu.VMEM((4, NP, PROWS, LANES), BF16),
        pltpu.VMEM((4 * AROWS, SEQ), BF16),
        pltpu.VMEM((8, UNIT * 48, LANES), BF16),
        pltpu.VMEM((48 * UNIT, PAIR), F32),
        pltpu.VMEM((HID * HID, PAIR), F32),
        pltpu.VMEM((HID * HID, PAIR), BF16),
        pltpu.VMEM((8, 4, RES * UNIT, PAIR), BF16),
        pltpu.VMEM((2, 2, 8, RES * UNIT, PAIR), BF16),
        pltpu.VMEM((4, 16, 256), F32),
        pltpu.VMEM((2, 2, 16, 256), F32),
        pltpu.VMEM((256, SEQ), BF16),
        pltpu.VMEM((2, 256, 16), F32),
        pltpu.VMEM((RES, 384, PAIR), F32),
        dma((9,)), dma((NP,)), dma,
        dma, dma((16, NP)), dma, dma((4, NP)), dma((2,)), dma((2, 2, 8)), dma((2,)), dma((2, 2)),
    ]

    def local_fn(m, mask, z, gamma, beta, w_a, b_a, w_b, b_b, w_out, b_out):
        out = pl.pallas_call(
            kernel,
            out_shape=pltpu.VMEM((RES, 384, PAIR), F32),
            in_specs=[any_spec] * 11,
            out_specs=vmem,
            scratch_shapes=scratch,
            compiler_params=pltpu.CompilerParams(
                collective_id=0, has_side_effects=True, vmem_limit_bytes=60 * 1024 * 1024),
            name="opm",
        )(jnp.transpose(m, (1, 0, 2)), mask.T, jnp.transpose(z, (1, 0, 2)), gamma, beta,
          w_a.T, b_a.reshape(1, HID), w_b.T, b_b.reshape(1, HID), w_out, b_out.reshape(1, PAIR))
        return jnp.transpose(out, (1, 0, 2))

    return jax.shard_map(local_fn, mesh=mesh, in_specs=in_specs, out_specs=row_spec, check_vma=False)
```

```python
import jax
import jax.numpy as jnp
from jax import lax
from jax.experimental import pallas as pl
from jax.experimental.pallas import tpu as pltpu
from jax.sharding import PartitionSpec as P

F32 = jnp.float32
BF16 = jnp.bfloat16
MESH = pl.DeviceIdType.MESH
NT = (((1,), (1,)), ((), ()))

SEQ, RES, CH, HID, PAIR = 512, 12, 256, 32, 128
LANES = 128
PIECE = 128
NP = SEQ // PIECE
AROWS = RES * HID
PROWS = AROWS + 16
UNIT = 2 * RES

WAYS = ("x+", "x-", "y+", "y-", "z+", "z-")
MOVE = {w: tuple((w[0] == ax) * (1 if w[1] == "+" else -1) for ax in "zyx") for w in WAYS}
STEPS = ((0, 0), (0, 1), (1, 0), (3, 0), (1, 1), (3, 1), (2, 0), (2, 1))


PLUS = {"x": (1, 2), "y": (2, 3), "z": (0, 1)}


def onward(place, p):
    dz, dy, dx = place

    def along(d, axis):
        if d == 1 and p in PLUS[axis]:
            return [axis + "+"]
        return [axis + "-"] if d == 3 and p not in PLUS[axis] else []

    if dz:
        return along(dz, "z")
    first, second, d1, d2 = ("y", "x", dy, dx) if p % 2 else ("x", "y", dx, dy)
    if d2:
        return along(d2, second)
    return along(d1, first) + [second + "+", second + "-"]


def all_hops():
    hops = [((0, 0, 0), p, way) for p in range(NP) for way in WAYS]
    for place, p, way in hops:
        to = tuple((a + b) % 4 for a, b in zip(place, MOVE[way]))
        for h in ((to, p, w) for w in onward(to, p)):
            if h not in hops:
                hops.append(h)
    return hops


ORDER = {-5: (0, 1, 2, 3, 4, 5), -4: (6, 7, 8, 9, 10), -3: (17,), -2: (12, 19, 14, 15, 22, 23), -1: (18, 13, 20, 21,
    16, 11, 26, 24, 28, 30, 31, 44, 32, 33, 27, 25, 37, 51, 38, 45, 39, 40, 47, 48, 41, 42, 49, 50, 46, 34), 1: (35,
    36, 60, 61), 2: (56, 66, 53, 55, 43, 54), 3: (57, 65, 62, 29, 59, 67), 4: (64, 58, 63, 52), 5: (69, 71, 70, 68)}


def iota(shape, axis):
    return lax.broadcasted_iota(jnp.int32, shape, axis)


def dot(a, b, dims=None):
    if dims is None:
        return jnp.dot(a, b, preferred_element_type=F32)
    return lax.dot_general(a, b, dims, preferred_element_type=F32)


def kernel(m_hbm, mask_hbm, z_hbm, gamma_hbm, beta_hbm, wa_hbm, ba_hbm, wb_hbm, bb_hbm, wo_hbm, bo_hbm,
           out_ref,
           mask_ref, gamma_ref, beta_ref, wa_ref, ba_ref, wb_ref, bb_ref, wo_ref, bo_ref,
           m_v, mask_v, wabig, b32, a_buf, b_buf, bt, lhs2, rt, w32, wo_p, r_send, r_recv, n_send, n_recv,
           mask_all, inv_v, z_v,
           in_sem, m_sem, z_sem, a_ss, a_rs, b_ss, b_rs, r_ss, r_rs, n_ss, n_rs):
    col = lax.axis_index("col")
    dap = lax.axis_index("dap")
    zz, yy, xx = col // 16, (col // 4) % 4, col % 4
    home = zz // 2
    other = 1 - dap

    def at(dz=0, dy=0, dx=0):
        return ((zz + dz) % 4) * 16 + ((yy + dy) % 4) * 4 + (xx + dx) % 4

    def dev(c, d):
        return {"col": c, "dap": d}

    small = [pltpu.make_async_copy(src, dst, in_sem.at[i]) for i, (src, dst) in enumerate((
        (mask_hbm, mask_ref), (gamma_hbm, gamma_ref), (beta_hbm, beta_ref), (wa_hbm, wa_ref), (ba_hbm, ba_ref),
        (wb_hbm, wb_ref), (bb_hbm, bb_ref), (wo_hbm, wo_ref), (bo_hbm, bo_ref)))]
    for p in range(NP):
        pltpu.make_async_copy(m_hbm.at[:, pl.ds(PIECE * p, PIECE), :], m_v.at[p], m_sem.at[p]).start()
        if p == 0:
            for copy in small:
                copy.start()
    barrier = pltpu.get_barrier_semaphore()
    greet = [dev(at(dy=1), dap), dev(at(dy=3), dap), dev(at(dx=1), dap), dev(at(dx=3), dap), dev(col, other)]
    for r in (1, 2, 3):
        for d in (0, 1):
            greet.append(dev(at(dz=r), d))
    for who in greet:
        pl.semaphore_signal(barrier, inc=1, device_id=who, device_id_type=MESH)

    for copy in small:
        copy.wait()
    mask_v[...] = jnp.zeros_like(mask_v)
    mask_v[0:RES, :] = mask_ref[...].astype(F32)
    wa = wa_ref[...]
    for k in range(4):
        rows = [wa if kk == k else jnp.zeros_like(wa) for kk in range(4)]
        wabig[:, CH * k:CH * (k + 1)] = jnp.concatenate(rows, axis=0)
    gamma = gamma_ref[...].astype(F32).reshape(1, CH)
    beta = beta_ref[...].astype(F32).reshape(1, CH)
    tile4 = jnp.where(iota((HID, LANES), 1) % HID == iota((HID, LANES), 0), 1.0, 0.0).astype(BF16)
    ba_row = dot(jnp.broadcast_to(ba_ref[...], (16, HID)), tile4)[0:1, :]
    eye = iota((HID, HID), 0) == iota((HID, HID), 1)
    bb_diag = jnp.where(eye, jnp.broadcast_to(bb_ref[...], (HID, HID)).astype(F32), 0.0).astype(BF16)
    bb_col = dot(bb_diag, jnp.ones((HID, LANES), BF16))

    def hop(place, p, way):
        to = tuple((d + s) % 4 for d, s in zip(place, MOVE[way]))
        if way[0] == "z":
            return pltpu.make_async_remote_copy(
                src_ref=b_buf.at[place[0], p], dst_ref=b_buf.at[to[0], p], send_sem=b_ss,
                recv_sem=b_rs.at[to[0], p], device_id=dev(at(*MOVE[way]), dap), device_id_type=MESH)
        src, dst = place[1] * 4 + place[2], to[1] * 4 + to[2]
        return pltpu.make_async_remote_copy(
            src_ref=a_buf.at[src, p], dst_ref=a_buf.at[dst, p], send_sem=a_ss,
            recv_sem=a_rs.at[dst, p], device_id=dev(at(*MOVE[way]), dap), device_id_type=MESH)

    def wait_a(i, p):
        pltpu.make_async_remote_copy(
            src_ref=a_buf.at[i, p], dst_ref=a_buf.at[i, p], send_sem=a_ss, recv_sem=a_rs.at[i, p],
            device_id=dev(at(dx=1), dap), device_id_type=MESH).wait_recv()

    def wait_b(r, p):
        pltpu.make_async_remote_copy(
            src_ref=b_buf.at[r, p], dst_ref=b_buf.at[r, p], send_sem=b_ss, recv_sem=b_rs.at[r, p],
            device_id=dev(at(dz=1), dap), device_id_type=MESH).wait_recv()

    hops = all_hops()
    seen = set()

    def need(place, p):
        if any(place) and (place, p) not in seen:
            seen.add((place, p))
            if place[0]:
                wait_b(place[0], p)
            else:
                wait_a(place[1] * 4 + place[2], p)

    def run(key):
        for i in ORDER.get(key, ()):
            place, p, way = hops[i]
            need(place, p)
            hop(place, p, way).start()

    def project(p, carry):
        pltpu.make_async_copy(m_hbm.at[:, pl.ds(0, PIECE), :], m_v.at[p], m_sem.at[p]).wait()
        lanes = pl.ds(pl.multiple_of(PIECE * p, PIECE), PIECE)
        mask_p = mask_v[:, lanes]
        mask_b = mask_p.astype(BF16)
        mask_t = mask_p.T.astype(BF16)
        for q in range(3):
            xs = []
            for k in range(4):
                n = 4 * q + k
                v = m_v[p, n].astype(F32)
                mean = jnp.sum(v, axis=1, keepdims=True) * (1.0 / CH)
                cen = v - mean
                var = jnp.sum(cen * cen, axis=1, keepdims=True) * (1.0 / CH)
                x = (cen * lax.rsqrt(var + 1e-5) * gamma + beta).astype(BF16)
                xs.append(x)
                lin_b = dot(wb_ref[...], x, NT)
                b32[pl.ds(n, HID, stride=RES), :] = (lin_b + bb_col) * mask_p[n:n + 1, :]
            lin_a = dot(jnp.concatenate(xs, axis=1), wabig[...], NT)
            spread = jnp.where(iota((16, LANES), 1) // HID + 4 * q == iota((16, LANES), 0), 1.0, 0.0).astype(BF16)
            a_buf[0, p, LANES * q:LANES * (q + 1), :] = ((lin_a + ba_row) * dot(mask_t, spread)).astype(BF16)
        a_buf[0, p, AROWS:PROWS, :] = mask_b
        b_buf[0, p, 0:AROWS, :] = b32[...].astype(BF16)
        b_buf[0, p, AROWS:PROWS, :] = mask_b

        @pl.when(p == 0)
        def _():
            pl.semaphore_wait(barrier, len(greet))

        for k in range(NP):
            @pl.when(p == k)
            def _(k=k):
                run(k - 5)
        return carry

    lax.fori_loop(0, NP, project, 0)
    pltpu.make_async_copy(z_hbm, z_v, z_sem).start()

    w32[...] = wo_ref[...].astype(F32)

    def order(d, carry):
        wo_p[pl.ds(pl.multiple_of(HID * d, HID), HID), :] = w32[pl.ds(d, HID, stride=HID), :].astype(BF16)
        return carry

    lax.fori_loop(0, HID, order, 0)

    run(-1)

    for r in (1, 3, 2):
        for p in range(NP):
            need((r, 0, 0), p)
    n192 = 4 * 4 * RES
    ro, co = iota((n192, n192), 0), iota((n192, n192), 1)
    want = ((ro // RES) % 4) * 48 + (ro // 48) * RES + ro % RES
    perm = jnp.where(want == co, 1.0, 0.0).astype(BF16)

    for g in range(8):
        cat = jnp.concatenate(
            [jnp.concatenate([b_buf[r, p, 48 * g:48 * (g + 1), :] for p in range(NP)], axis=1) for r in range(4)], axis=0)
        bt[n192 * g:n192 * (g + 1), :] = dot(perm, cat).astype(BF16)

    lane = iota((1, LANES), 1)
    low = lane < 64
    odd = (lane // HID) % 2 == 1

    def transpose4(v):
        def swap(u, w):
            t = pltpu.roll(jnp.where(low, w, u), 64, 1)
            return jnp.where(low, u, t), jnp.where(low, t, w)

        def swap2(u, w):
            return (jnp.where(odd, pltpu.roll(w, 32, 1), u), jnp.where(odd, w, pltpu.roll(u, 96, 1)))

        e0, e2 = swap(v[0], v[2])
        e1, e3 = swap(v[1], v[3])
        w0, w1 = swap2(e0, e1)
        w2, w3 = swap2(e2, e3)
        return w0, w1, w2, w3

    def r_copy(t, r, unit):
        return pltpu.make_async_remote_copy(
            src_ref=r_send.at[t, r], dst_ref=r_recv.at[zz % 2, dap, unit], send_sem=r_ss.at[1 if r else 0],
            recv_sem=r_rs.at[zz % 2, dap, unit], device_id=dev(at(dz=-r), home), device_id_type=MESH)

    def n_copy(r):
        return pltpu.make_async_remote_copy(
            src_ref=n_send.at[r], dst_ref=n_recv.at[zz % 2, dap], send_sem=n_ss.at[1 if r else 0],
            recv_sem=n_rs.at[zz % 2, dap], device_id=dev(at(dz=-r), home), device_id_type=MESH)

    def count():
        for dy in range(4):
            for dx in range(4):
                pos = ((yy + 4 - dy) % 4) * 4 + (xx + 4 - dx) % 4
                mask_all[pl.ds(pl.multiple_of(16 * pos, 16), 16), :] = jnp.concatenate(
                    [a_buf[dy * 4 + dx, p, AROWS:PROWS, :] for p in range(NP)], axis=1)
        ro, co = iota((256, 256), 0), iota((256, 256), 1)
        squeeze = jnp.where((ro < 192) & ((ro // RES) * 16 + ro % RES == co), 1.0, 0.0).astype(BF16)
        mask_rows = dot(squeeze, mask_all[...]).astype(BF16)
        for r in range(4):
            mask_cols = jnp.concatenate([b_buf[r, p, AROWS:PROWS, :] for p in range(NP)], axis=1)
            part = dot(mask_cols, mask_rows, NT)
            if r:
                n_send[r] = part
                n_copy(r).start()
            else:
                @pl.when(home == dap)
                def _(part=part):
                    n_recv[zz % 2, dap] = part

                @pl.when(home != dap)
                def _(part=part):
                    n_send[0] = part
                    n_copy(0).start()

    stay = [p for d in (1, 3) for p in (1, 3) if not onward((0, 1, d), p)]
    px = 3 - 2 * (xx % 2)

    def place(t):
        dy, far = jnp.int32(STEPS[7][0]), jnp.int32(STEPS[7][1])
        for i in range(6, -1, -1):
            dy = jnp.where(t == i, STEPS[i][0], dy)
            far = jnp.where(t == i, STEPS[i][1], far)
        pair = (xx // 2 + far) % 2
        return dy, pair, ((yy + 4 - dy) % 4) * 2 + pair

    def step(t, carry):
        for at_t in range(8):
            @pl.when(t == at_t)
            def _(at_t=at_t):
                run(at_t)
                dy, far = STEPS[at_t]
                rest = [p for p in (0, 2) if dy and not onward((0, dy, 1), p)]
                for dx in (2 * far, 1, 3):
                    for p in range(NP):
                        if onward((0, dy, dx), p):
                            need((0, dy, dx), p)
                near = 4 - px if far else px
                for p in rest + [1, 3] * far:
                    if dy or far:
                        wait_a(dy * 4 + 2 * far, p)
                for q in rest:
                    wait_a(dy * 4 + near, q)
                wait_a(dy * 4 + near, jnp.where(near == 1, stay[0], stay[1]))
                if at_t == 7:
                    count()

        dy, pair, unit = place(t)
        slots = [dy * 4 + (xx + 4 - (2 * pair + o)) % 4 for o in range(2)]

        for c in range(3):
            quads = (2 * c, 2 * c + 1)
            rhs = jnp.concatenate(
                [jnp.concatenate([a_buf[slots[q // 3], p, LANES * (q % 3):LANES * (q % 3 + 1), :] for q in quads], axis=1)
                 for p in range(NP)], axis=0)
            for g in range(2):
                prod = dot(bt[4 * n192 * g:4 * n192 * (g + 1), :], rhs)
                for h in range(4):
                    for k2, q in enumerate(quads):
                        base = n192 * h
                        v = [prod[base + 48 * d:base + 48 * (d + 1), LANES * k2:LANES * (k2 + 1)] for d in range(4)]
                        for k, w in enumerate(transpose4(v)):
                            i = 4 * q + k
                            lhs2[4 * g + h, 48 * i:48 * (i + 1), :] = w.astype(BF16)
        res = dot(jnp.concatenate([lhs2[g] for g in range(8)], axis=1), wo_p[...])
        for i in range(UNIT):
            for jg in range(6):
                rt[pl.ds(8 * jg * UNIT + i, 8, stride=UNIT), :] = res[48 * i + 8 * jg:48 * i + 8 * jg + 8, :]
        own = rt[0:RES * UNIT, :].astype(BF16)

        @pl.when(home == dap)
        def _():
            r_recv[zz % 2, dap, unit] = own

        for r in (2, 1, 3):
            r_send[t, r] = rt[RES * UNIT * r:RES * UNIT * (r + 1), :].astype(BF16)
            r_copy(t, r, unit).start()

        @pl.when(home != dap)
        def _():
            r_send[t, 0] = own
            r_copy(t, 0, unit).start()
        return carry

    lax.fori_loop(0, 8, step, 0)

    pltpu.make_async_copy(z_hbm, z_v, z_sem).wait()
    bo = bo_ref[...].astype(F32)

    def arrive(ref, sem, src):
        pltpu.make_async_remote_copy(
            src_ref=src, dst_ref=ref, send_sem=n_ss.at[0], recv_sem=sem,
            device_id=dev(col, other), device_id_type=MESH).wait_recv()

    for k in range(2):
        for c in range(2):
            @pl.when(jnp.logical_not((zz == 2 * dap + k) & (dap == c)))
            def _(k=k, c=c):
                arrive(n_recv.at[k, c], n_rs.at[k, c], n_send.at[0])
        inv = 1.0 / (1e-3 + (n_recv[k, 0] + n_recv[k, 1]))
        inv_v[k] = inv.T

    def finish(t, carry):
        _, _, u = place(t)
        for k in range(2):
            for c in range(2):
                @pl.when(jnp.logical_not((zz == 2 * dap + k) & (dap == c)))
                def _(k=k, c=c):
                    arrive(r_recv.at[k, c, u], r_rs.at[k, c, u], r_send.at[0, 0])
        for k in range(2):
            rows = pl.ds(pl.multiple_of(UNIT * u, 8), UNIT)
            dst = pl.ds(pl.multiple_of(192 * k + UNIT * u, 8), UNIT)
            inv = inv_v[k, rows, :]
            total = r_recv[k, 0, u].astype(F32) + r_recv[k, 1, u].astype(F32) + bo
            for j in range(RES):
                out_ref[j, dst, :] = z_v[j, dst, :] + total[UNIT * j:UNIT * (j + 1), :] * inv[:, j:j + 1]
        return carry

    lax.fori_loop(0, 8, finish, 0)

    def left(ref, sem):
        pltpu.make_async_remote_copy(src_ref=ref, dst_ref=ref, send_sem=sem, recv_sem=n_rs.at[0, 0],
                                     device_id=dev(col, other), device_id_type=MESH).wait_send()

    left(a_buf.at[pl.ds(0, 15)], a_ss)
    left(b_buf.at[pl.ds(0, 3)], b_ss)
    left(r_send.at[pl.ds(0, 6)], r_ss.at[1])
    left(n_send.at[pl.ds(0, 3)], n_ss.at[1])

    @pl.when(home != dap)
    def _():
        left(r_send.at[pl.ds(0, 2)], r_ss.at[0])
        left(n_send.at[pl.ds(0, 1)], n_ss.at[0])


def solution(mesh):
    row_spec = P(("data", "dap"), "col", None)
    mask_spec = P(("data", "dap"), "col")
    in_specs = (row_spec, mask_spec, row_spec) + (P(),) * 8
    any_spec = pl.BlockSpec(memory_space=pl.ANY)
    vmem = pl.BlockSpec(memory_space=pltpu.VMEM)
    dma = pltpu.SemaphoreType.DMA
    scratch = [
        pltpu.VMEM((RES, SEQ), jnp.int32), pltpu.VMEM((CH,), BF16), pltpu.VMEM((CH,), BF16), pltpu.VMEM((HID, CH), BF16),
        pltpu.VMEM((1, HID), BF16), pltpu.VMEM((HID, CH), BF16), pltpu.VMEM((1, HID), BF16),
        pltpu.VMEM((HID * HID, PAIR), BF16), pltpu.VMEM((1, PAIR), BF16),
        pltpu.VMEM((NP, RES, PIECE, CH), BF16),
        pltpu.VMEM((16, SEQ), F32),
        pltpu.VMEM((LANES, 4 * CH), BF16),
        pltpu.VMEM((AROWS, PIECE), F32),
        pltpu.VMEM((16, NP, PROWS, LANES), BF16),
        pltpu.VMEM((4, NP, PROWS, LANES), BF16),
        pltpu.VMEM((4 * AROWS, SEQ), BF16),
        pltpu.VMEM((8, UNIT * 48, LANES), BF16),
        pltpu.VMEM((48 * UNIT, PAIR), F32),
        pltpu.VMEM((HID * HID, PAIR), F32),
        pltpu.VMEM((HID * HID, PAIR), BF16),
        pltpu.VMEM((8, 4, RES * UNIT, PAIR), BF16),
        pltpu.VMEM((2, 2, 8, RES * UNIT, PAIR), BF16),
        pltpu.VMEM((4, 16, 256), F32),
        pltpu.VMEM((2, 2, 16, 256), F32),
        pltpu.VMEM((256, SEQ), BF16),
        pltpu.VMEM((2, 256, 16), F32),
        pltpu.VMEM((RES, 384, PAIR), F32),
        dma((9,)), dma((NP,)), dma,
        dma, dma((16, NP)), dma, dma((4, NP)), dma((2,)), dma((2, 2, 8)), dma((2,)), dma((2, 2)),
    ]

    def local_fn(m, mask, z, gamma, beta, w_a, b_a, w_b, b_b, w_out, b_out):
        out = pl.pallas_call(
            kernel,
            out_shape=pltpu.VMEM((RES, 384, PAIR), F32),
            in_specs=[any_spec] * 11,
            out_specs=vmem,
            scratch_shapes=scratch,
            compiler_params=pltpu.CompilerParams(
                collective_id=0, has_side_effects=True, vmem_limit_bytes=60 * 1024 * 1024),
            name="opm",
        )(jnp.transpose(m, (1, 0, 2)), mask.T, jnp.transpose(z, (1, 0, 2)), gamma, beta,
          w_a.T, b_a.reshape(1, HID), w_b.T, b_b.reshape(1, HID), w_out, b_out.reshape(1, PAIR))
        return jnp.transpose(out, (1, 0, 2))

    return jax.shard_map(local_fn, mesh=mesh, in_specs=in_specs, out_specs=row_spec, check_vma=False)
```

```python
import jax
import jax.numpy as jnp
from jax import lax
from jax.experimental import pallas as pl
from jax.experimental.pallas import tpu as pltpu
from jax.sharding import PartitionSpec as P

F32 = jnp.float32
BF16 = jnp.bfloat16
MESH = pl.DeviceIdType.MESH
NT = (((1,), (1,)), ((), ()))

SEQ, RES, CH, HID, PAIR = 512, 12, 256, 32, 128
LANES = 128
PIECE = 128
NP = SEQ // PIECE
AROWS = RES * HID
PROWS = AROWS + 16
UNIT = 2 * RES

WAYS = ("x+", "x-", "y+", "y-", "z+", "z-")
MOVE = {w: tuple((w[0] == ax) * (1 if w[1] == "+" else -1) for ax in "zyx") for w in WAYS}
STEPS = ((0, 0), (0, 1), (1, 0), (3, 0), (1, 1), (3, 1), (2, 0), (2, 1))


PLUS = {"x": (1, 2), "y": (2, 3), "z": (0, 1)}


def onward(place, p):
    dz, dy, dx = place

    def along(d, axis):
        if d == 1 and p in PLUS[axis]:
            return [axis + "+"]
        return [axis + "-"] if d == 3 and p not in PLUS[axis] else []

    if dz:
        return along(dz, "z")
    first, second, d1, d2 = ("y", "x", dy, dx) if p % 2 else ("x", "y", dx, dy)
    if d2:
        return along(d2, second)
    return along(d1, first) + [second + "+", second + "-"]


def all_hops():
    hops = [((0, 0, 0), p, way) for p in range(NP) for way in WAYS]
    for place, p, way in hops:
        to = tuple((a + b) % 4 for a, b in zip(place, MOVE[way]))
        for h in ((to, p, w) for w in onward(to, p)):
            if h not in hops:
                hops.append(h)
    return hops


OWN = sorted({(place, p) for place, p, _ in all_hops() if any(place)})


ORDER = {-5: (0, 1, 2, 3, 4, 5), -4: (6, 7, 8, 9, 10), -3: (17,), -2: (12, 19, 14, 15, 22, 23), -1: (18, 13, 20, 21,
    16, 11, 26, 24, 28, 30, 31, 44, 32, 33, 27, 25, 37, 51, 38, 45, 39, 40, 47, 48, 41, 42, 49, 50, 46, 34), 1: (35,
    36, 60, 61), 2: (56, 66, 53, 55, 43, 54), 3: (57, 65, 62, 29, 59, 67), 4: (64, 58, 63, 52), 5: (69, 71, 70, 68)}


def iota(shape, axis):
    return lax.broadcasted_iota(jnp.int32, shape, axis)


def dot(a, b, dims=None):
    if dims is None:
        return jnp.dot(a, b, preferred_element_type=F32)
    return lax.dot_general(a, b, dims, preferred_element_type=F32)


def kernel(m_hbm, mask_hbm, z_hbm, gamma_hbm, beta_hbm, wa_hbm, ba_hbm, wb_hbm, bb_hbm, wo_hbm, bo_hbm,
           out_ref,
           mask_ref, gamma_ref, beta_ref, wa_ref, ba_ref, wb_ref, bb_ref, wo_ref, bo_ref,
           m_v, mask_v, wabig, b32, a_buf, b_buf, bt, lhs2, rt, w32, wo_p, r_send, r_recv, n_send, n_recv,
           mask_all, inv_v, z_v,
           in_sem, m_sem, z_sem, a_ss, a_rs, own_rs, b_ss, b_rs, r_ss, r_rs, n_ss, n_rs):
    col = lax.axis_index("col")
    dap = lax.axis_index("dap")
    zz, yy, xx = col // 16, (col // 4) % 4, col % 4
    home = zz // 2
    other = 1 - dap

    def at(dz=0, dy=0, dx=0):
        return ((zz + dz) % 4) * 16 + ((yy + dy) % 4) * 4 + (xx + dx) % 4

    def dev(c, d):
        return {"col": c, "dap": d}

    small = [pltpu.make_async_copy(src, dst, in_sem.at[i]) for i, (src, dst) in enumerate((
        (mask_hbm, mask_ref), (gamma_hbm, gamma_ref), (beta_hbm, beta_ref), (wa_hbm, wa_ref), (ba_hbm, ba_ref),
        (wb_hbm, wb_ref), (bb_hbm, bb_ref), (wo_hbm, wo_ref), (bo_hbm, bo_ref)))]
    for p in range(NP):
        pltpu.make_async_copy(m_hbm.at[:, pl.ds(PIECE * p, PIECE), :], m_v.at[p], m_sem.at[p]).start()
        if p == 0:
            for copy in small:
                copy.start()
    barrier = pltpu.get_barrier_semaphore()
    greet = [dev(at(dy=1), dap), dev(at(dy=3), dap), dev(at(dx=1), dap), dev(at(dx=3), dap), dev(col, other)]
    for r in (1, 2, 3):
        for d in (0, 1):
            greet.append(dev(at(dz=r), d))
    for who in greet:
        pl.semaphore_signal(barrier, inc=1, device_id=who, device_id_type=MESH)

    for copy in small:
        copy.wait()
    mask_v[...] = jnp.zeros_like(mask_v)
    mask_v[0:RES, :] = mask_ref[...].astype(F32)
    wa = wa_ref[...]
    for k in range(4):
        rows = [wa if kk == k else jnp.zeros_like(wa) for kk in range(4)]
        wabig[:, CH * k:CH * (k + 1)] = jnp.concatenate(rows, axis=0)
    gamma = gamma_ref[...].astype(F32).reshape(1, CH)
    beta = beta_ref[...].astype(F32).reshape(1, CH)
    tile4 = jnp.where(iota((HID, LANES), 1) % HID == iota((HID, LANES), 0), 1.0, 0.0).astype(BF16)
    ba_row = dot(jnp.broadcast_to(ba_ref[...], (16, HID)), tile4)[0:1, :]
    eye = iota((HID, HID), 0) == iota((HID, HID), 1)
    bb_diag = jnp.where(eye, jnp.broadcast_to(bb_ref[...], (HID, HID)).astype(F32), 0.0).astype(BF16)
    bb_col = dot(bb_diag, jnp.ones((HID, LANES), BF16))

    def landed(place, p):
        if onward(place, p):
            return own_rs.at[OWN.index((place, p))]
        return b_rs.at[place[0]] if place[0] else a_rs.at[place[1] * 4 + place[2]]

    def hop(place, p, way):
        to = tuple((d + s) % 4 for d, s in zip(place, MOVE[way]))
        if way[0] == "z":
            return pltpu.make_async_remote_copy(
                src_ref=b_buf.at[place[0], p], dst_ref=b_buf.at[to[0], p], send_sem=b_ss,
                recv_sem=landed(to, p), device_id=dev(at(*MOVE[way]), dap), device_id_type=MESH)
        src, dst = place[1] * 4 + place[2], to[1] * 4 + to[2]
        return pltpu.make_async_remote_copy(
            src_ref=a_buf.at[src, p], dst_ref=a_buf.at[dst, p], send_sem=a_ss,
            recv_sem=landed(to, p), device_id=dev(at(*MOVE[way]), dap), device_id_type=MESH)

    def wait(ref, sem):
        pltpu.make_async_remote_copy(src_ref=ref, dst_ref=ref, send_sem=a_ss, recv_sem=sem,
                                     device_id=dev(at(dx=1), dap), device_id_type=MESH).wait_recv()

    hops = all_hops()
    seen = set()

    def need(place, p):
        if any(place) and (place, p) not in seen:
            seen.add((place, p))
            buf = b_buf.at[place[0], p] if place[0] else a_buf.at[place[1] * 4 + place[2], p]
            wait(buf, landed(place, p))

    def run(key):
        for i in ORDER.get(key, ()):
            place, p, way = hops[i]
            need(place, p)
            hop(place, p, way).start()

    def project(p, carry):
        pltpu.make_async_copy(m_hbm.at[:, pl.ds(0, PIECE), :], m_v.at[p], m_sem.at[p]).wait()
        lanes = pl.ds(pl.multiple_of(PIECE * p, PIECE), PIECE)
        mask_p = mask_v[:, lanes]
        mask_b = mask_p.astype(BF16)
        mask_t = mask_p.T.astype(BF16)
        for q in range(3):
            xs = []
            for k in range(4):
                n = 4 * q + k
                v = m_v[p, n].astype(F32)
                mean = jnp.sum(v, axis=1, keepdims=True) * (1.0 / CH)
                cen = v - mean
                var = jnp.sum(cen * cen, axis=1, keepdims=True) * (1.0 / CH)
                x = (cen * lax.rsqrt(var + 1e-5) * gamma + beta).astype(BF16)
                xs.append(x)
                lin_b = dot(wb_ref[...], x, NT)
                b32[pl.ds(n, HID, stride=RES), :] = (lin_b + bb_col) * mask_p[n:n + 1, :]
            lin_a = dot(jnp.concatenate(xs, axis=1), wabig[...], NT)
            spread = jnp.where(iota((16, LANES), 1) // HID + 4 * q == iota((16, LANES), 0), 1.0, 0.0).astype(BF16)
            a_buf[0, p, LANES * q:LANES * (q + 1), :] = ((lin_a + ba_row) * dot(mask_t, spread)).astype(BF16)
        a_buf[0, p, AROWS:PROWS, :] = mask_b
        b_buf[0, p, 0:AROWS, :] = b32[...].astype(BF16)
        b_buf[0, p, AROWS:PROWS, :] = mask_b

        @pl.when(p == 0)
        def _():
            pl.semaphore_wait(barrier, len(greet))

        for k in range(NP):
            @pl.when(p == k)
            def _(k=k):
                run(k - 5)
        return carry

    lax.fori_loop(0, NP, project, 0)
    pltpu.make_async_copy(z_hbm, z_v, z_sem).start()

    w32[...] = wo_ref[...].astype(F32)

    def order(d, carry):
        wo_p[pl.ds(pl.multiple_of(HID * d, HID), HID), :] = w32[pl.ds(d, HID, stride=HID), :].astype(BF16)
        return carry

    lax.fori_loop(0, HID, order, 0)

    run(-1)

    for r in (1, 3, 2):
        for p in range(NP):
            if onward((r, 0, 0), p):
                need((r, 0, 0), p)
        wait(b_buf.at[r, pl.ds(0, NP if r == 2 else NP // 2)], b_rs.at[r])
    n192 = 4 * 4 * RES
    ro, co = iota((n192, n192), 0), iota((n192, n192), 1)
    want = ((ro // RES) % 4) * 48 + (ro // 48) * RES + ro % RES
    perm = jnp.where(want == co, 1.0, 0.0).astype(BF16)

    for g in range(8):
        cat = jnp.concatenate(
            [jnp.concatenate([b_buf[r, p, 48 * g:48 * (g + 1), :] for p in range(NP)], axis=1) for r in range(4)], axis=0)
        bt[n192 * g:n192 * (g + 1), :] = dot(perm, cat).astype(BF16)

    lane = iota((1, LANES), 1)
    low = lane < 64
    odd = (lane // HID) % 2 == 1

    def transpose4(v):
        def swap(u, w):
            t = pltpu.roll(jnp.where(low, w, u), 64, 1)
            return jnp.where(low, u, t), jnp.where(low, t, w)

        def swap2(u, w):
            return (jnp.where(odd, pltpu.roll(w, 32, 1), u), jnp.where(odd, w, pltpu.roll(u, 96, 1)))

        e0, e2 = swap(v[0], v[2])
        e1, e3 = swap(v[1], v[3])
        w0, w1 = swap2(e0, e1)
        w2, w3 = swap2(e2, e3)
        return w0, w1, w2, w3

    def r_copy(t, r, unit):
        return pltpu.make_async_remote_copy(
            src_ref=r_send.at[t, r], dst_ref=r_recv.at[zz % 2, dap, unit], send_sem=r_ss.at[1 if r else 0],
            recv_sem=r_rs.at[zz % 2, unit], device_id=dev(at(dz=-r), home), device_id_type=MESH)

    def n_copy(r):
        return pltpu.make_async_remote_copy(
            src_ref=n_send.at[r], dst_ref=n_recv.at[zz % 2, dap], send_sem=n_ss.at[1 if r else 0],
            recv_sem=n_rs.at[zz % 2], device_id=dev(at(dz=-r), home), device_id_type=MESH)

    def count():
        for dy in range(4):
            for dx in range(4):
                pos = ((yy + 4 - dy) % 4) * 4 + (xx + 4 - dx) % 4
                mask_all[pl.ds(pl.multiple_of(16 * pos, 16), 16), :] = jnp.concatenate(
                    [a_buf[dy * 4 + dx, p, AROWS:PROWS, :] for p in range(NP)], axis=1)
        ro, co = iota((256, 256), 0), iota((256, 256), 1)
        squeeze = jnp.where((ro < 192) & ((ro // RES) * 16 + ro % RES == co), 1.0, 0.0).astype(BF16)
        mask_rows = dot(squeeze, mask_all[...]).astype(BF16)
        for r in range(4):
            mask_cols = jnp.concatenate([b_buf[r, p, AROWS:PROWS, :] for p in range(NP)], axis=1)
            part = dot(mask_cols, mask_rows, NT)
            if r:
                n_send[r] = part
                n_copy(r).start()
            else:
                @pl.when(home == dap)
                def _(part=part):
                    n_recv[zz % 2, dap] = part

                @pl.when(home != dap)
                def _(part=part):
                    n_send[0] = part
                    n_copy(0).start()

    px = 3 - 2 * (xx % 2)

    def place(t):
        dy, far = jnp.int32(STEPS[7][0]), jnp.int32(STEPS[7][1])
        for i in range(6, -1, -1):
            dy = jnp.where(t == i, STEPS[i][0], dy)
            far = jnp.where(t == i, STEPS[i][1], far)
        pair = (xx // 2 + far) % 2
        return dy, pair, ((yy + 4 - dy) % 4) * 2 + pair

    def step(t, carry):
        for at_t in range(8):
            @pl.when(t == at_t)
            def _(at_t=at_t):
                run(at_t)
                dy, far = STEPS[at_t]
                rest = [p for p in (0, 2) if dy and not onward((0, dy, 1), p)]
                for dx in (2 * far, 1, 3):
                    for p in range(NP):
                        if onward((0, dy, dx), p):
                            need((0, dy, dx), p)
                near = dy * 4 + (4 - px if far else px)
                kept = len(rest) + 2 * far
                if kept:
                    wait(a_buf.at[dy * 4 + 2 * far, pl.ds(0, kept)], a_rs.at[dy * 4 + 2 * far])
                wait(a_buf.at[near, pl.ds(0, len(rest) + 1)], a_rs.at[near])
                if at_t == 7:
                    count()

        dy, pair, unit = place(t)
        slots = [dy * 4 + (xx + 4 - (2 * pair + o)) % 4 for o in range(2)]

        for c in range(3):
            quads = (2 * c, 2 * c + 1)
            rhs = jnp.concatenate(
                [jnp.concatenate([a_buf[slots[q // 3], p, LANES * (q % 3):LANES * (q % 3 + 1), :] for q in quads], axis=1)
                 for p in range(NP)], axis=0)
            for g in range(2):
                prod = dot(bt[4 * n192 * g:4 * n192 * (g + 1), :], rhs)
                for h in range(4):
                    for k2, q in enumerate(quads):
                        base = n192 * h
                        v = [prod[base + 48 * d:base + 48 * (d + 1), LANES * k2:LANES * (k2 + 1)] for d in range(4)]
                        for k, w in enumerate(transpose4(v)):
                            i = 4 * q + k
                            lhs2[4 * g + h, 48 * i:48 * (i + 1), :] = w.astype(BF16)
        res = dot(jnp.concatenate([lhs2[g] for g in range(8)], axis=1), wo_p[...])
        for i in range(UNIT):
            for jg in range(6):
                rt[pl.ds(8 * jg * UNIT + i, 8, stride=UNIT), :] = res[48 * i + 8 * jg:48 * i + 8 * jg + 8, :]
        own = rt[0:RES * UNIT, :].astype(BF16)

        @pl.when(home == dap)
        def _():
            r_recv[zz % 2, dap, unit] = own

        for r in (2, 1, 3):
            r_send[t, r] = rt[RES * UNIT * r:RES * UNIT * (r + 1), :].astype(BF16)
            r_copy(t, r, unit).start()

        @pl.when(home != dap)
        def _():
            r_send[t, 0] = own
            r_copy(t, 0, unit).start()
        return carry

    lax.fori_loop(0, 8, step, 0)

    pltpu.make_async_copy(z_hbm, z_v, z_sem).wait()
    bo = bo_ref[...].astype(F32)

    def arrive(k, whole, part, sem):
        @pl.when(zz != 2 * dap + k)
        def _():
            wait(whole, sem)

        @pl.when(zz == 2 * dap + k)
        def _():
            wait(part, sem)

    for k in range(2):
        arrive(k, n_recv.at[k], n_recv.at[k, other], n_rs.at[k])
        inv = 1.0 / (1e-3 + (n_recv[k, 0] + n_recv[k, 1]))
        inv_v[k] = inv.T

    def finish(t, carry):
        _, _, u = place(t)
        for k in range(2):
            arrive(k, r_recv.at[k, pl.ds(0, 2), u], r_recv.at[k, other, u], r_rs.at[k, u])
        for k in range(2):
            rows = pl.ds(pl.multiple_of(UNIT * u, 8), UNIT)
            dst = pl.ds(pl.multiple_of(192 * k + UNIT * u, 8), UNIT)
            inv = inv_v[k, rows, :]
            total = r_recv[k, 0, u].astype(F32) + r_recv[k, 1, u].astype(F32) + bo
            for j in range(RES):
                out_ref[j, dst, :] = z_v[j, dst, :] + total[UNIT * j:UNIT * (j + 1), :] * inv[:, j:j + 1]
        return carry

    lax.fori_loop(0, 8, finish, 0)

    def left(ref, sem):
        pltpu.make_async_remote_copy(src_ref=ref, dst_ref=ref, send_sem=sem, recv_sem=n_rs.at[0],
                                     device_id=dev(col, other), device_id_type=MESH).wait_send()

    left(a_buf.at[pl.ds(0, 15)], a_ss)
    left(b_buf.at[pl.ds(0, 3)], b_ss)
    left(r_send.at[pl.ds(0, 6)], r_ss.at[1])
    left(n_send.at[pl.ds(0, 3)], n_ss.at[1])

    @pl.when(home != dap)
    def _():
        left(r_send.at[pl.ds(0, 2)], r_ss.at[0])
        left(n_send.at[pl.ds(0, 1)], n_ss.at[0])


def solution(mesh):
    row_spec = P(("data", "dap"), "col", None)
    mask_spec = P(("data", "dap"), "col")
    in_specs = (row_spec, mask_spec, row_spec) + (P(),) * 8
    any_spec = pl.BlockSpec(memory_space=pl.ANY)
    vmem = pl.BlockSpec(memory_space=pltpu.VMEM)
    dma = pltpu.SemaphoreType.DMA
    scratch = [
        pltpu.VMEM((RES, SEQ), jnp.int32), pltpu.VMEM((CH,), BF16), pltpu.VMEM((CH,), BF16), pltpu.VMEM((HID, CH), BF16),
        pltpu.VMEM((1, HID), BF16), pltpu.VMEM((HID, CH), BF16), pltpu.VMEM((1, HID), BF16),
        pltpu.VMEM((HID * HID, PAIR), BF16), pltpu.VMEM((1, PAIR), BF16),
        pltpu.VMEM((NP, RES, PIECE, CH), BF16),
        pltpu.VMEM((16, SEQ), F32),
        pltpu.VMEM((LANES, 4 * CH), BF16),
        pltpu.VMEM((AROWS, PIECE), F32),
        pltpu.VMEM((16, NP, PROWS, LANES), BF16),
        pltpu.VMEM((4, NP, PROWS, LANES), BF16),
        pltpu.VMEM((4 * AROWS, SEQ), BF16),
        pltpu.VMEM((8, UNIT * 48, LANES), BF16),
        pltpu.VMEM((48 * UNIT, PAIR), F32),
        pltpu.VMEM((HID * HID, PAIR), F32),
        pltpu.VMEM((HID * HID, PAIR), BF16),
        pltpu.VMEM((8, 4, RES * UNIT, PAIR), BF16),
        pltpu.VMEM((2, 2, 8, RES * UNIT, PAIR), BF16),
        pltpu.VMEM((4, 16, 256), F32),
        pltpu.VMEM((2, 2, 16, 256), F32),
        pltpu.VMEM((256, SEQ), BF16),
        pltpu.VMEM((2, 256, 16), F32),
        pltpu.VMEM((RES, 384, PAIR), F32),
        dma((9,)), dma((NP,)), dma,
        dma, dma((16,)), dma((len(OWN),)), dma, dma((4,)), dma((2,)), dma((2, 8)), dma((2,)), dma((2,)),
    ]

    def local_fn(m, mask, z, gamma, beta, w_a, b_a, w_b, b_b, w_out, b_out):
        out = pl.pallas_call(
            kernel,
            out_shape=pltpu.VMEM((RES, 384, PAIR), F32),
            in_specs=[any_spec] * 11,
            out_specs=vmem,
            scratch_shapes=scratch,
            compiler_params=pltpu.CompilerParams(
                collective_id=0, has_side_effects=True, vmem_limit_bytes=60 * 1024 * 1024),
            name="opm",
        )(jnp.transpose(m, (1, 0, 2)), mask.T, jnp.transpose(z, (1, 0, 2)), gamma, beta,
          w_a.T, b_a.reshape(1, HID), w_b.T, b_b.reshape(1, HID), w_out, b_out.reshape(1, PAIR))
        return jnp.transpose(out, (1, 0, 2))

    return jax.shard_map(local_fn, mesh=mesh, in_specs=in_specs, out_specs=row_spec, check_vma=False)
```

```python
import jax
import jax.numpy as jnp
from jax import lax
from jax.experimental import pallas as pl
from jax.experimental.pallas import tpu as pltpu
from jax.sharding import PartitionSpec as P

F32 = jnp.float32
BF16 = jnp.bfloat16
MESH = pl.DeviceIdType.MESH
NT = (((1,), (1,)), ((), ()))

SEQ, RES, CH, HID, PAIR = 512, 12, 256, 32, 128
LANES = 128
PIECE = 128
NP = SEQ // PIECE
AROWS = RES * HID
PROWS = AROWS + 16
UNIT = 2 * RES

WAYS = ("x+", "x-", "y+", "y-", "z+", "z-")
MOVE = {w: tuple((w[0] == ax) * (1 if w[1] == "+" else -1) for ax in "zyx") for w in WAYS}
STEPS = ((0, 0), (0, 1), (1, 0), (3, 0), (1, 1), (3, 1), (2, 0), (2, 1))


PLUS = {"x": (1, 2), "y": (2, 3), "z": (0, 1)}


def onward(place, p):
    dz, dy, dx = place

    def along(d, axis):
        if d == 1 and p in PLUS[axis]:
            return [axis + "+"]
        return [axis + "-"] if d == 3 and p not in PLUS[axis] else []

    if dz:
        return along(dz, "z")
    first, second, d1, d2 = ("y", "x", dy, dx) if p % 2 else ("x", "y", dx, dy)
    if d2:
        return along(d2, second)
    return along(d1, first) + [second + "+", second + "-"]


def all_hops():
    hops = [((0, 0, 0), p, way) for p in range(NP) for way in WAYS]
    for place, p, way in hops:
        to = tuple((a + b) % 4 for a, b in zip(place, MOVE[way]))
        for h in ((to, p, w) for w in onward(to, p)):
            if h not in hops:
                hops.append(h)
    return hops


OWN = sorted({(place, p) for place, p, _ in all_hops() if any(place)})


ORDER = {-5: (0, 1, 2, 3, 4, 5), -4: (6, 7, 8, 9, 10), -3: (17,), -2: (12, 19, 14, 15, 22, 23), -1: (18, 13, 20, 21,
    16, 11, 26, 24, 28, 30, 31, 44, 32, 33, 27, 25, 37, 51, 38, 45, 39, 40, 47, 48, 41, 42, 49, 50, 46, 34), 1: (35,
    36, 60, 61), 2: (56, 66, 53, 55, 43, 54), 3: (57, 65, 62, 29, 59, 67), 4: (64, 58, 63, 52), 5: (69, 71, 70, 68)}


def iota(shape, axis):
    return lax.broadcasted_iota(jnp.int32, shape, axis)


def dot(a, b, dims=None):
    if dims is None:
        return jnp.dot(a, b, preferred_element_type=F32)
    return lax.dot_general(a, b, dims, preferred_element_type=F32)


def kernel(m_hbm, mask_hbm, z_hbm, gamma_hbm, beta_hbm, wa_hbm, ba_hbm, wb_hbm, bb_hbm, wo_hbm, bo_hbm,
           out_ref,
           mask_ref, gamma_ref, beta_ref, wa_ref, ba_ref, wb_ref, bb_ref, wo_ref, bo_ref,
           m_v, mask_v, wabig, b32, a_buf, b_buf, bt, lhs2, rt, w32, wo_p, r_send, r_recv, n_send, n_recv,
           mask_all, inv_v, z_v, squeeze_v,
           in_sem, m_sem, z_sem, a_ss, a_rs, own_rs, b_ss, b_rs, r_ss, r_rs, n_ss, n_rs):
    col = lax.axis_index("col")
    dap = lax.axis_index("dap")
    zz, yy, xx = col // 16, (col // 4) % 4, col % 4
    home = zz // 2
    other = 1 - dap

    def at(dz=0, dy=0, dx=0):
        return ((zz + dz) % 4) * 16 + ((yy + dy) % 4) * 4 + (xx + dx) % 4

    def dev(c, d):
        return {"col": c, "dap": d}

    small = [pltpu.make_async_copy(src, dst, in_sem.at[i]) for i, (src, dst) in enumerate((
        (mask_hbm, mask_ref), (gamma_hbm, gamma_ref), (beta_hbm, beta_ref), (wa_hbm, wa_ref), (ba_hbm, ba_ref),
        (wb_hbm, wb_ref), (bb_hbm, bb_ref), (wo_hbm, wo_ref), (bo_hbm, bo_ref)))]
    for p in range(NP):
        pltpu.make_async_copy(m_hbm.at[:, pl.ds(PIECE * p, PIECE), :], m_v.at[p], m_sem.at[p]).start()
        if p == 0:
            for copy in small:
                copy.start()
    barrier = pltpu.get_barrier_semaphore()
    greet = [dev(at(dy=1), dap), dev(at(dy=3), dap), dev(at(dx=1), dap), dev(at(dx=3), dap), dev(col, other)]
    for r in (1, 2, 3):
        for d in (0, 1):
            greet.append(dev(at(dz=r), d))
    for who in greet:
        pl.semaphore_signal(barrier, inc=1, device_id=who, device_id_type=MESH)

    for copy in small:
        copy.wait()
    mask_v[...] = jnp.zeros_like(mask_v)
    mask_v[0:RES, :] = mask_ref[...].astype(F32)
    wa = wa_ref[...]
    for k in range(4):
        rows = [wa if kk == k else jnp.zeros_like(wa) for kk in range(4)]
        wabig[:, CH * k:CH * (k + 1)] = jnp.concatenate(rows, axis=0)
    gamma = gamma_ref[...].astype(F32).reshape(1, CH)
    beta = beta_ref[...].astype(F32).reshape(1, CH)
    tile4 = jnp.where(iota((HID, LANES), 1) % HID == iota((HID, LANES), 0), 1.0, 0.0).astype(BF16)
    ba_row = dot(jnp.broadcast_to(ba_ref[...], (16, HID)), tile4)[0:1, :]
    eye = iota((HID, HID), 0) == iota((HID, HID), 1)
    bb_diag = jnp.where(eye, jnp.broadcast_to(bb_ref[...], (HID, HID)).astype(F32), 0.0).astype(BF16)
    bb_col = dot(bb_diag, jnp.ones((HID, LANES), BF16))

    def landed(place, p):
        if onward(place, p):
            return own_rs.at[OWN.index((place, p))]
        return b_rs.at[place[0]] if place[0] else a_rs.at[place[1] * 4 + place[2]]

    def hop(place, p, way):
        to = tuple((d + s) % 4 for d, s in zip(place, MOVE[way]))
        if way[0] == "z":
            return pltpu.make_async_remote_copy(
                src_ref=b_buf.at[place[0], p], dst_ref=b_buf.at[to[0], p], send_sem=b_ss,
                recv_sem=landed(to, p), device_id=dev(at(*MOVE[way]), dap), device_id_type=MESH)
        src, dst = place[1] * 4 + place[2], to[1] * 4 + to[2]
        return pltpu.make_async_remote_copy(
            src_ref=a_buf.at[src, p], dst_ref=a_buf.at[dst, p], send_sem=a_ss,
            recv_sem=landed(to, p), device_id=dev(at(*MOVE[way]), dap), device_id_type=MESH)

    def wait(ref, sem):
        pltpu.make_async_remote_copy(src_ref=ref, dst_ref=ref, send_sem=a_ss, recv_sem=sem,
                                     device_id=dev(at(dx=1), dap), device_id_type=MESH).wait_recv()

    hops = all_hops()
    seen = set()

    def need(place, p):
        if any(place) and (place, p) not in seen:
            seen.add((place, p))
            buf = b_buf.at[place[0], p] if place[0] else a_buf.at[place[1] * 4 + place[2], p]
            wait(buf, landed(place, p))

    def run(key):
        for i in ORDER.get(key, ()):
            place, p, way = hops[i]
            need(place, p)
            hop(place, p, way).start()

    def project(p, carry):
        pltpu.make_async_copy(m_hbm.at[:, pl.ds(0, PIECE), :], m_v.at[p], m_sem.at[p]).wait()
        lanes = pl.ds(pl.multiple_of(PIECE * p, PIECE), PIECE)
        mask_p = mask_v[:, lanes]
        mask_b = mask_p.astype(BF16)
        mask_t = mask_p.T.astype(BF16)
        for q in range(3):
            xs = []
            for k in range(4):
                n = 4 * q + k
                v = m_v[p, n].astype(F32)
                mean = jnp.sum(v, axis=1, keepdims=True) * (1.0 / CH)
                cen = v - mean
                var = jnp.sum(cen * cen, axis=1, keepdims=True) * (1.0 / CH)
                x = (cen * lax.rsqrt(var + 1e-5) * gamma + beta).astype(BF16)
                xs.append(x)
                lin_b = dot(wb_ref[...], x, NT)
                b32[pl.ds(n, HID, stride=RES), :] = (lin_b + bb_col) * mask_p[n:n + 1, :]
            lin_a = dot(jnp.concatenate(xs, axis=1), wabig[...], NT)
            spread = jnp.where(iota((16, LANES), 1) // HID + 4 * q == iota((16, LANES), 0), 1.0, 0.0).astype(BF16)
            a_buf[0, p, LANES * q:LANES * (q + 1), :] = ((lin_a + ba_row) * dot(mask_t, spread)).astype(BF16)
        a_buf[0, p, AROWS:PROWS, :] = mask_b
        b_buf[0, p, 0:AROWS, :] = b32[...].astype(BF16)
        b_buf[0, p, AROWS:PROWS, :] = mask_b

        @pl.when(p == 0)
        def _():
            pl.semaphore_wait(barrier, len(greet))

        for k in range(NP):
            @pl.when(p == k)
            def _(k=k):
                run(k - 5)
        return carry

    lax.fori_loop(0, NP, project, 0)
    pltpu.make_async_copy(z_hbm, z_v, z_sem).start()

    w32[...] = wo_ref[...].astype(F32)

    def order(d, carry):
        wo_p[pl.ds(pl.multiple_of(HID * d, HID), HID), :] = w32[pl.ds(d, HID, stride=HID), :].astype(BF16)
        return carry

    lax.fori_loop(0, HID, order, 0)

    ro, co = iota((256, 256), 0), iota((256, 256), 1)
    squeeze_v[...] = jnp.where((ro < 192) & ((ro // RES) * 16 + ro % RES == co), 1.0, 0.0).astype(BF16)
    run(-1)

    for r in (1, 3, 2):
        for p in range(NP):
            if onward((r, 0, 0), p):
                need((r, 0, 0), p)
        wait(b_buf.at[r, pl.ds(0, NP if r == 2 else NP // 2)], b_rs.at[r])
    n192 = 4 * 4 * RES
    ro, co = iota((n192, n192), 0), iota((n192, n192), 1)
    want = ((ro // RES) % 4) * 48 + (ro // 48) * RES + ro % RES
    perm = jnp.where(want == co, 1.0, 0.0).astype(BF16)

    for g in range(8):
        cat = jnp.concatenate(
            [jnp.concatenate([b_buf[r, p, 48 * g:48 * (g + 1), :] for p in range(NP)], axis=1) for r in range(4)], axis=0)
        bt[n192 * g:n192 * (g + 1), :] = dot(perm, cat).astype(BF16)

    lane = iota((1, LANES), 1)
    low = lane < 64
    odd = (lane // HID) % 2 == 1

    def transpose4(v):
        def swap(u, w):
            t = pltpu.roll(jnp.where(low, w, u), 64, 1)
            return jnp.where(low, u, t), jnp.where(low, t, w)

        def swap2(u, w):
            return (jnp.where(odd, pltpu.roll(w, 32, 1), u), jnp.where(odd, w, pltpu.roll(u, 96, 1)))

        e0, e2 = swap(v[0], v[2])
        e1, e3 = swap(v[1], v[3])
        w0, w1 = swap2(e0, e1)
        w2, w3 = swap2(e2, e3)
        return w0, w1, w2, w3

    def r_copy(t, r, unit):
        return pltpu.make_async_remote_copy(
            src_ref=r_send.at[t, r], dst_ref=r_recv.at[zz % 2, dap, unit], send_sem=r_ss.at[1 if r else 0],
            recv_sem=r_rs.at[zz % 2, unit], device_id=dev(at(dz=-r), home), device_id_type=MESH)

    def n_copy(r):
        return pltpu.make_async_remote_copy(
            src_ref=n_send.at[r], dst_ref=n_recv.at[zz % 2, dap], send_sem=n_ss.at[1 if r else 0],
            recv_sem=n_rs.at[zz % 2], device_id=dev(at(dz=-r), home), device_id_type=MESH)

    def gather_masks(lines):
        for dy in lines:
            for dx in range(4):
                pos = ((yy + 4 - dy) % 4) * 4 + (xx + 4 - dx) % 4
                mask_all[pl.ds(pl.multiple_of(16 * pos, 16), 16), :] = jnp.concatenate(
                    [a_buf[dy * 4 + dx, p, AROWS:PROWS, :] for p in range(NP)], axis=1)

    def count():
        gather_masks((STEPS[7][0],))
        mask_rows = dot(squeeze_v[...], mask_all[...]).astype(BF16)
        for r in range(4):
            mask_cols = jnp.concatenate([b_buf[r, p, AROWS:PROWS, :] for p in range(NP)], axis=1)
            part = dot(mask_cols, mask_rows, NT)
            if r:
                n_send[r] = part
                n_copy(r).start()
            else:
                @pl.when(home == dap)
                def _(part=part):
                    n_recv[zz % 2, dap] = part

                @pl.when(home != dap)
                def _(part=part):
                    n_send[0] = part
                    n_copy(0).start()

    px = 3 - 2 * (xx % 2)

    def place(t):
        dy, far = jnp.int32(STEPS[7][0]), jnp.int32(STEPS[7][1])
        for i in range(6, -1, -1):
            dy = jnp.where(t == i, STEPS[i][0], dy)
            far = jnp.where(t == i, STEPS[i][1], far)
        pair = (xx // 2 + far) % 2
        return dy, pair, ((yy + 4 - dy) % 4) * 2 + pair

    def step(t, carry):
        for at_t in range(8):
            @pl.when(t == at_t)
            def _(at_t=at_t):
                run(at_t)
                dy, far = STEPS[at_t]
                rest = [p for p in (0, 2) if dy and not onward((0, dy, 1), p)]
                for dx in (2 * far, 1, 3):
                    for p in range(NP):
                        if onward((0, dy, dx), p):
                            need((0, dy, dx), p)
                near = dy * 4 + (4 - px if far else px)
                kept = len(rest) + 2 * far
                if kept:
                    wait(a_buf.at[dy * 4 + 2 * far, pl.ds(0, kept)], a_rs.at[dy * 4 + 2 * far])
                wait(a_buf.at[near, pl.ds(0, len(rest) + 1)], a_rs.at[near])
                if at_t == 6:
                    gather_masks([d for d in range(4) if d != dy])
                if at_t == 7:
                    count()

        dy, pair, unit = place(t)
        slots = [dy * 4 + (xx + 4 - (2 * pair + o)) % 4 for o in range(2)]

        for c in range(3):
            quads = (2 * c, 2 * c + 1)
            rhs = jnp.concatenate(
                [jnp.concatenate([a_buf[slots[q // 3], p, LANES * (q % 3):LANES * (q % 3 + 1), :] for q in quads], axis=1)
                 for p in range(NP)], axis=0)
            for g in range(2):
                prod = dot(bt[4 * n192 * g:4 * n192 * (g + 1), :], rhs)
                for h in range(4):
                    for k2, q in enumerate(quads):
                        base = n192 * h
                        v = [prod[base + 48 * d:base + 48 * (d + 1), LANES * k2:LANES * (k2 + 1)] for d in range(4)]
                        for k, w in enumerate(transpose4(v)):
                            i = 4 * q + k
                            lhs2[4 * g + h, 48 * i:48 * (i + 1), :] = w.astype(BF16)
        res = dot(jnp.concatenate([lhs2[g] for g in range(8)], axis=1), wo_p[...])
        for i in range(UNIT):
            for jg in range(6):
                rt[pl.ds(8 * jg * UNIT + i, 8, stride=UNIT), :] = res[48 * i + 8 * jg:48 * i + 8 * jg + 8, :]
        own = rt[0:RES * UNIT, :].astype(BF16)

        @pl.when(home == dap)
        def _():
            r_recv[zz % 2, dap, unit] = own

        for r in (2, 1, 3):
            r_send[t, r] = rt[RES * UNIT * r:RES * UNIT * (r + 1), :].astype(BF16)
            r_copy(t, r, unit).start()

        @pl.when(home != dap)
        def _():
            r_send[t, 0] = own
            r_copy(t, 0, unit).start()
        return carry

    lax.fori_loop(0, 8, step, 0)

    pltpu.make_async_copy(z_hbm, z_v, z_sem).wait()
    bo = bo_ref[...].astype(F32)

    def arrive(k, whole, part, sem):
        @pl.when(zz != 2 * dap + k)
        def _():
            wait(whole, sem)

        @pl.when(zz == 2 * dap + k)
        def _():
            wait(part, sem)

    for k in range(2):
        arrive(k, n_recv.at[k], n_recv.at[k, other], n_rs.at[k])
        inv = 1.0 / (1e-3 + (n_recv[k, 0] + n_recv[k, 1]))
        inv_v[k] = inv.T

    def finish(t, carry):
        _, _, u = place(t)
        for k in range(2):
            arrive(k, r_recv.at[k, pl.ds(0, 2), u], r_recv.at[k, other, u], r_rs.at[k, u])
        for k in range(2):
            rows = pl.ds(pl.multiple_of(UNIT * u, 8), UNIT)
            dst = pl.ds(pl.multiple_of(192 * k + UNIT * u, 8), UNIT)
            inv = inv_v[k, rows, :]
            total = r_recv[k, 0, u].astype(F32) + r_recv[k, 1, u].astype(F32) + bo
            for j in range(RES):
                out_ref[j, dst, :] = z_v[j, dst, :] + total[UNIT * j:UNIT * (j + 1), :] * inv[:, j:j + 1]
        return carry

    lax.fori_loop(0, 8, finish, 0)

    def left(ref, sem):
        pltpu.make_async_remote_copy(src_ref=ref, dst_ref=ref, send_sem=sem, recv_sem=n_rs.at[0],
                                     device_id=dev(col, other), device_id_type=MESH).wait_send()

    left(a_buf.at[pl.ds(0, 15)], a_ss)
    left(b_buf.at[pl.ds(0, 3)], b_ss)
    left(r_send.at[pl.ds(0, 6)], r_ss.at[1])
    left(n_send.at[pl.ds(0, 3)], n_ss.at[1])

    @pl.when(home != dap)
    def _():
        left(r_send.at[pl.ds(0, 2)], r_ss.at[0])
        left(n_send.at[pl.ds(0, 1)], n_ss.at[0])


def solution(mesh):
    row_spec = P(("data", "dap"), "col", None)
    mask_spec = P(("data", "dap"), "col")
    in_specs = (row_spec, mask_spec, row_spec) + (P(),) * 8
    any_spec = pl.BlockSpec(memory_space=pl.ANY)
    vmem = pl.BlockSpec(memory_space=pltpu.VMEM)
    dma = pltpu.SemaphoreType.DMA
    scratch = [
        pltpu.VMEM((RES, SEQ), jnp.int32), pltpu.VMEM((CH,), BF16), pltpu.VMEM((CH,), BF16), pltpu.VMEM((HID, CH), BF16),
        pltpu.VMEM((1, HID), BF16), pltpu.VMEM((HID, CH), BF16), pltpu.VMEM((1, HID), BF16),
        pltpu.VMEM((HID * HID, PAIR), BF16), pltpu.VMEM((1, PAIR), BF16),
        pltpu.VMEM((NP, RES, PIECE, CH), BF16),
        pltpu.VMEM((16, SEQ), F32),
        pltpu.VMEM((LANES, 4 * CH), BF16),
        pltpu.VMEM((AROWS, PIECE), F32),
        pltpu.VMEM((16, NP, PROWS, LANES), BF16),
        pltpu.VMEM((4, NP, PROWS, LANES), BF16),
        pltpu.VMEM((4 * AROWS, SEQ), BF16),
        pltpu.VMEM((8, UNIT * 48, LANES), BF16),
        pltpu.VMEM((48 * UNIT, PAIR), F32),
        pltpu.VMEM((HID * HID, PAIR), F32),
        pltpu.VMEM((HID * HID, PAIR), BF16),
        pltpu.VMEM((8, 4, RES * UNIT, PAIR), BF16),
        pltpu.VMEM((2, 2, 8, RES * UNIT, PAIR), BF16),
        pltpu.VMEM((4, 16, 256), F32),
        pltpu.VMEM((2, 2, 16, 256), F32),
        pltpu.VMEM((256, SEQ), BF16),
        pltpu.VMEM((2, 256, 16), F32),
        pltpu.VMEM((RES, 384, PAIR), F32), pltpu.VMEM((256, 256), BF16),
        dma((9,)), dma((NP,)), dma,
        dma, dma((16,)), dma((len(OWN),)), dma, dma((4,)), dma((2,)), dma((2, 8)), dma((2,)), dma((2,)),
    ]

    def local_fn(m, mask, z, gamma, beta, w_a, b_a, w_b, b_b, w_out, b_out):
        out = pl.pallas_call(
            kernel,
            out_shape=pltpu.VMEM((RES, 384, PAIR), F32),
            in_specs=[any_spec] * 11,
            out_specs=vmem,
            scratch_shapes=scratch,
            compiler_params=pltpu.CompilerParams(
                collective_id=0, has_side_effects=True, vmem_limit_bytes=60 * 1024 * 1024),
            name="opm",
        )(jnp.transpose(m, (1, 0, 2)), mask.T, jnp.transpose(z, (1, 0, 2)), gamma, beta,
          w_a.T, b_a.reshape(1, HID), w_b.T, b_b.reshape(1, HID), w_out, b_out.reshape(1, PAIR))
        return jnp.transpose(out, (1, 0, 2))

    return jax.shard_map(local_fn, mesh=mesh, in_specs=in_specs, out_specs=row_spec, check_vma=False)
```
